32 devices in a mesh: groups: 2 (over y), pair: 4 (over z), tp: 4 (over x, core).
Axes of the slice: x: 2, y: 2, z: 4, core: 2. Of those that a mesh axis runs over, the one named last changes fastest.
Arguments:
- prompt_keys: bfloat16 [8, 1536, 8, 128], P(('groups', 'pair'), None, 'tp'), parts along dimension 0, may hold values from -6 to 6
- prompt_values: bfloat16 [8, 1536, 8, 128], P(('groups', 'pair'), None, 'tp'), parts along dimension 0, may hold values from -6 to 6
- span_queries: bfloat16 [8, 512, 64, 128], P(('groups', 'pair'), None, 'tp'), parts along dimension 0, may hold values from -1024 to 1024
- span_keys: bfloat16 [8, 512, 8, 128], P(('groups', 'pair'), None, 'tp'), parts along dimension 0, may hold values from -6 to 6
- span_values: bfloat16 [8, 512, 8, 128], P(('groups', 'pair'), None, 'tp'), parts along dimension 0, may hold values from -6 to 6
- prefill_residual: bfloat16 [8, 512, 8192], P(('groups', 'pair'), None, 'tp'), parts along dimension 0, may hold values from -8 to 8
- decode_queries: bfloat16 [8, 2, 32, 64, 128], P(('groups', 'pair'), None, None, 'tp'), parts along dimension 0, may hold values from -1024 to 1024
- decode_keys: bfloat16 [8, 2, 32, 8, 128], P(('groups', 'pair'), None, None, 'tp'), parts along dimension 0, may hold values from -16 to 16
- decode_values: bfloat16 [8, 2, 32, 8, 128], P(('groups', 'pair'), None, None, 'tp'), parts along dimension 0, may hold values from -6 to 6
- decode_residual: bfloat16 [8, 2, 32, 8192], P(('groups', 'pair'), None, None, 'tp'), parts along dimension 0, may hold values from -8 to 8
- cursor: int32 [8, 32], P(('groups', 'pair')), parts along dimension 0, may hold values from 1024 to 2048
- norm_gain: bfloat16 [8192], P('tp'), may hold values from 0.25 to 1.75
Outputs:
- prefill_normed: bfloat16 [8, 512, 8192], P(('groups', 'pair'), None, 'tp'), parts along dimension 0
- handed_keys: bfloat16 [8, 2048, 8, 128], P(('groups', 'pair'), None, 'tp'), parts along dimension 0
- handed_values: bfloat16 [8, 2048, 8, 128], P(('groups', 'pair'), None, 'tp'), parts along dimension 0
- decode_normed: bfloat16 [8, 2, 32, 8192], P(('groups', 'pair'), None, None, 'tp'), parts along dimension 0
The draws below stay inside these ranges and needn't reach their ends.
There are 2 independent parts, one for each index of `groups`. The reference program is written for one: setup_inputs(seed, part) draws one part's arguments, and reference() takes and returns one part's arrays. A program takes and returns all parts, laid end to end along the dimension named above; an argument that names none is the same for every part. Nothing has to cross between parts.
All inputs are finite; a program needn't handle non-finite values.
Results may differ from the reference program's by a relative error of at most 0.0034.
Values may be sent and summed in bfloat16 or wider, within the bound.
No kernel may reach another device: no remote copies, remote signals or barrier semaphores. Data moves between devices by JAX's collectives and lax.ppermute only.
A program may use at most 128 MiB of HBM per device.

```python
import jax
import jax.numpy as jnp
from jax import lax

D = 8192
H = 64
KVH = 8
HD = 128
S = 2048
SPAN = 512
ROWS = 32
STEPS = 2
NPROMPT = 4
CTX = 1536


def clipped_normal(key, array_shape):
    return jnp.clip(jax.random.normal(key, array_shape, jnp.float32), -6.0, 6.0)


def cache_keys(key):
    array_shape = (NPROMPT, CTX, KVH, HD)
    return clipped_normal(jax.random.fold_in(key, 101), array_shape)


def draw_prompt_keys(key, part):
    return cache_keys(key).astype(jnp.bfloat16)


def draw_span_queries(key, part):
    base_draw = clipped_normal(jax.random.fold_in(key, 201), (NPROMPT, SPAN, H, HD))
    return base_draw.astype(jnp.bfloat16)


def decode_base(key):
    return clipped_normal(jax.random.fold_in(key, 301), (NPROMPT, STEPS, ROWS, H, HD))


def draw_decode_queries(key, part):
    base_draw = decode_base(key)
    return base_draw.astype(jnp.bfloat16)


def draw_decode_keys(key, part):
    groups = H // KVH
    base_draw = decode_base(key).reshape(NPROMPT, STEPS, ROWS, KVH, groups, HD)
    summed = jnp.sum(base_draw, axis=4) * (1.2 / groups ** 0.5)
    jitter_term = clipped_normal(jax.random.fold_in(key, 303), summed.shape)
    return (summed + 0.3 * jitter_term).astype(jnp.bfloat16)


def spread_rows(key, array_shape):
    feature_count = array_shape[-1]
    position = jnp.arange(feature_count, dtype=jnp.float32) / (feature_count - 1)
    row_shape = array_shape[:-1] + (1,)
    entries = clipped_normal(jax.random.fold_in(key, 1), array_shape)
    feature_trend = 3.0 ** (0.5 * position)
    column_spread = 10.0 ** (0.5 * jax.random.uniform(jax.random.fold_in(key, 2), (feature_count,), jnp.float32))
    row_spread = 10.0 ** (0.5 * jax.random.uniform(jax.random.fold_in(key, 3), row_shape, jnp.float32))
    return 0.03 * entries * feature_trend * column_spread * row_spread


def draw_prefill_residual(key, part):
    return spread_rows(jax.random.fold_in(key, 401), (NPROMPT, SPAN, D)).astype(jnp.bfloat16)


def draw_decode_residual(key, part):
    return spread_rows(jax.random.fold_in(key, 501), (NPROMPT, STEPS, ROWS, D)).astype(jnp.bfloat16)


def place_ends(result, key, least, high):
    place = [jax.random.randint(jax.random.fold_in(key, axis), (), 0, length) for axis, length in enumerate(result.shape)]
    main_axis = result.shape.index(max(result.shape))
    neighbour = place[:main_axis] + [(place[main_axis] + 1) % result.shape[main_axis]] + place[main_axis + 1:]
    return result.at[tuple(place)].set(least).at[tuple(neighbour)].set(high)


def steps_of(stream_key, dims, split, smallest, top_value):
    loudness = 1.0
    for axis_at, shards_of in split:
        steps = jax.random.uniform(jax.random.fold_in(jax.random.fold_in(stream_key, 6), axis_at), (shards_of,), jnp.float32, smallest / len(split), top_value / len(split))
        loudness = loudness * jnp.repeat(jnp.exp(steps), dims[axis_at] // shards_of).reshape((-1,) + (1,) * (len(dims) - 1 - axis_at))
    return loudness


def gaussian(own_key, dims, spread, limit, cuts=(), held_as=jnp.bfloat16):
    drawn = jax.random.normal(own_key, dims, jnp.float32) * spread
    if len(cuts) > 0:
        drawn = steps_of(own_key, dims, cuts, -0.22, 0.18) * drawn
    return jnp.clip(drawn, min=-limit, max=limit).astype(held_as)


def setup_inputs(seed: int = 0, part: int = 0) -> dict:
    splits = jax.random.split(jax.random.key(seed), 13)
    part_splits = jax.random.split(jax.random.fold_in(splits[12], part), 13)
    return {
        "prompt_keys": draw_prompt_keys(jax.random.fold_in(jax.random.fold_in(splits[12], part), 71), part),
        "prompt_values": gaussian(part_splits[1], (NPROMPT, CTX, KVH, HD), 1.0, 6.0, ((0, 4), (2, 4))),
        "span_queries": draw_span_queries(jax.random.fold_in(jax.random.fold_in(splits[12], part), 71), part),
        "span_keys": gaussian(part_splits[3], (NPROMPT, SPAN, KVH, HD), 1.0, 6.0, ((0, 4), (2, 4))),
        "span_values": gaussian(part_splits[4], (NPROMPT, SPAN, KVH, HD), 1.0, 6.0, ((0, 4), (2, 4))),
        "prefill_residual": draw_prefill_residual(jax.random.fold_in(jax.random.fold_in(splits[12], part), 71), part),
        "decode_queries": draw_decode_queries(jax.random.fold_in(jax.random.fold_in(splits[12], part), 71), part),
        "decode_keys": draw_decode_keys(jax.random.fold_in(jax.random.fold_in(splits[12], part), 71), part),
        "decode_values": gaussian(part_splits[8], (NPROMPT, STEPS, ROWS, KVH, HD), 1.0, 6.0, ((0, 4), (3, 4))),
        "decode_residual": draw_decode_residual(jax.random.fold_in(jax.random.fold_in(splits[12], part), 71), part),
        "cursor": place_ends(jax.random.randint(part_splits[10], (NPROMPT, ROWS), S // 2, S + 1), jax.random.fold_in(part_splits[10], 1), S // 2, S).astype(jnp.int32),
        "norm_gain": jnp.clip(1.0 + 0.15 * jax.random.normal(splits[11], (D,), jnp.float32), 0.25, 1.75).astype(jnp.bfloat16),
    }


epsilon = 1e-05

def normalize(hidden, gain_wide):
    squares = lax.optimization_barrier(jnp.mean(hidden * hidden, axis=-1, keepdims=True))
    return (hidden * lax.rsqrt(squares + epsilon) * gain_wide).astype(jnp.bfloat16)

def prefill_attention(queries, keys_one, values_one):
    span_len = queries.shape[0]
    query_heads = queries.shape[1]
    head_size = queries.shape[2]
    key_heads = keys_one.shape[1]
    positions = keys_one.shape[0]
    groups = query_heads // key_heads
    score_scale = head_size ** (-0.5)
    row_index = jnp.arange(span_len, dtype=jnp.int32)[:, None] + (positions - span_len)
    col_index = jnp.arange(positions, dtype=jnp.int32)[None, :]
    visible = col_index <= row_index

    def one_head(head_index):
        query = lax.dynamic_index_in_dim(queries, head_index, 1, keepdims=False)
        key_head = lax.dynamic_index_in_dim(keys_one, head_index // groups, 1, keepdims=False)
        value_head = lax.dynamic_index_in_dim(values_one, head_index // groups, 1, keepdims=False)
        scores = jnp.dot(query, key_head.T, preferred_element_type=jnp.float32) * score_scale
        scores = jnp.where(visible, scores, -jnp.inf)
        row_max = lax.optimization_barrier(jnp.max(scores, axis=1, keepdims=True))
        scaled = jnp.exp(scores - row_max)
        denominator = lax.optimization_barrier(jnp.sum(scaled, axis=1, keepdims=True))
        weights = scaled.astype(jnp.bfloat16)
        return jnp.dot(weights, value_head, preferred_element_type=jnp.float32) / denominator
    per_head = lax.map(one_head, jnp.arange(query_heads, dtype=jnp.int32))
    return jnp.transpose(per_head, (1, 0, 2)).reshape(span_len, query_heads * head_size)

def decode_attention(queries, own_keys, own_values, reach_count, keys_one, values_one):
    steps_count, row_count, query_heads, head_size = queries.shape
    key_heads = keys_one.shape[1]
    positions = keys_one.shape[0]
    groups = query_heads // key_heads
    score_scale = head_size ** (-0.5)
    grouped = queries.astype(jnp.float32).reshape(steps_count, row_count, key_heads, groups, head_size)
    far_scores = jnp.einsum('trkgd,skd->trkgs', grouped, keys_one.astype(jnp.float32)) * score_scale
    reach = jnp.arange(positions, dtype=jnp.int32)[None, :] < reach_count[:, None]
    far_scores = jnp.where(reach[None, :, None, None, :], far_scores, -jnp.inf)
    own_scores = jnp.einsum('trkgd,urkd->trkgu', grouped, own_keys.astype(jnp.float32)) * score_scale
    earlier = jnp.arange(steps_count)[None, :] <= jnp.arange(steps_count)[:, None]
    own_scores = jnp.where(earlier[:, None, None, None, :], own_scores, -jnp.inf)
    row_max = jnp.maximum(lax.optimization_barrier(jnp.max(far_scores, axis=4)), lax.optimization_barrier(jnp.max(own_scores, axis=4)))[..., None]
    far_expon = jnp.exp(far_scores - row_max)
    own_expon = jnp.exp(own_scores - row_max)
    denominator = lax.optimization_barrier(jnp.sum(far_expon, axis=4)) + lax.optimization_barrier(jnp.sum(own_expon, axis=4))
    far_weights = far_expon.astype(jnp.bfloat16).astype(jnp.float32)
    own_weights = own_expon.astype(jnp.bfloat16).astype(jnp.float32)
    attended = jnp.einsum('trkgs,skd->trkgd', far_weights, values_one.astype(jnp.float32))
    attended = attended + jnp.einsum('trkgu,urkd->trkgd', own_weights, own_values.astype(jnp.float32))
    attended = attended / denominator[..., None]
    return attended.reshape(steps_count, row_count, query_heads * head_size)

def reference(prompt_keys, prompt_values, span_queries, span_keys, span_values, prefill_residual, decode_queries, decode_keys, decode_values, decode_residual, cursor, norm_gain):
    keys_all = jnp.concatenate([prompt_keys, span_keys], axis=1)
    values_all = jnp.concatenate([prompt_values, span_values], axis=1)
    gain_wide = norm_gain.astype(jnp.float32)

    def prefill_one(inputs):
        queries, keys_one, values_one, residual = inputs
        hidden = prefill_attention(queries, keys_one, values_one) + residual.astype(jnp.float32)
        return normalize(hidden, gain_wide)
    prefill_normed = lax.map(prefill_one, (span_queries, keys_all, values_all, prefill_residual))
    handed_keys = jnp.roll(keys_all, -(NPROMPT // 2), axis=0)
    handed_values = jnp.roll(values_all, -(NPROMPT // 2), axis=0)

    def decode_one(inputs):
        queries, own_keys, own_values, reach_count, keys_one, values_one, residual = inputs
        hidden = decode_attention(queries, own_keys, own_values, reach_count, keys_one, values_one) + residual.astype(jnp.float32)
        return normalize(hidden, gain_wide)
    decode_normed = lax.map(decode_one, (decode_queries, decode_keys, decode_values, cursor, handed_keys, handed_values, decode_residual))
    return (prefill_normed, handed_keys, handed_values, decode_normed)
```

```python
import functools

import jax
import jax.numpy as jnp
from jax import lax
from jax.experimental import pallas as pl
from jax.experimental.pallas import tpu as pltpu
from jax.sharding import PartitionSpec as P

epsilon = 1e-05
log2_e = 1.4426950408889634


def from_behind(value, axis, steps):
    count = lax.axis_size(axis)
    pairs = [(source, (source + steps) % count) for source in range(count)]
    return lax.ppermute(value, axis, pairs)


def sum_over(value, axis):
    count = lax.axis_size(axis)
    if count & (count - 1):
        return lax.psum(value, axis)
    step = 1
    while step < count:
        value = value + lax.ppermute(value, axis, [(i, i ^ step) for i in range(count)])
        step *= 2
    return value


def contract_last(a, b):
    return lax.dot_general(a, b, (((1,), (1,)), ((), ())), preferred_element_type=jnp.float32)


def prefill_kernel(q_ref, k_ref, v_ref, residual_ref, hidden_ref, squares_ref, *, block, past):
    rows = q_ref.shape[1]
    head_size = q_ref.shape[2]
    factor = head_size ** (-0.5) * log2_e

    @pl.when(pl.program_id(0) == 0)
    def _():
        squares_ref[...] = jnp.zeros_like(squares_ref)

    visible = lax.broadcasted_iota(jnp.int32, (block, block), 1) <= lax.broadcasted_iota(
        jnp.int32, (block, block), 0
    )
    for start in range(0, rows, block):
        here = slice(start, start + block)
        before = past + start
        q = q_ref[0, here]
        far = contract_last(q, k_ref[0, :before])
        near = contract_last(q, k_ref[0, before : before + block])
        near = jnp.where(visible, near, -jnp.inf)
        top = jnp.maximum(
            jnp.max(far, axis=1, keepdims=True), jnp.max(near, axis=1, keepdims=True)
        )
        far = jnp.exp2((far - top) * factor)
        near = jnp.exp2((near - top) * factor)
        total = jnp.sum(far, axis=1, keepdims=True) + jnp.sum(near, axis=1, keepdims=True)
        mixed = jnp.dot(
            far.astype(jnp.bfloat16), v_ref[0, :before], preferred_element_type=jnp.float32
        ) + jnp.dot(
            near.astype(jnp.bfloat16),
            v_ref[0, before : before + block],
            preferred_element_type=jnp.float32,
        )
        hidden = mixed / total + residual_ref[here].astype(jnp.float32)
        hidden_ref[here] = hidden
        squares_ref[here] = squares_ref[here] + hidden * hidden


def prefill(queries, keys, values, residual):
    heads, rows, head_size = queries.shape
    key_heads, positions, _ = keys.shape
    per = heads // key_heads
    block = 256 if rows % 256 == 0 else rows
    return pl.pallas_call(
        functools.partial(prefill_kernel, block=block, past=positions - rows),
        grid=(heads,),
        in_specs=[
            pl.BlockSpec((1, rows, head_size), lambda h: (h, 0, 0)),
            pl.BlockSpec((1, positions, head_size), lambda h: (h // per, 0, 0)),
            pl.BlockSpec((1, positions, head_size), lambda h: (h // per, 0, 0)),
            pl.BlockSpec((rows, head_size), lambda h: (0, h)),
        ],
        out_specs=[
            pl.BlockSpec((rows, head_size), lambda h: (0, h)),
            pl.BlockSpec((rows, head_size), lambda h: (0, 0)),
        ],
        out_shape=[
            jax.ShapeDtypeStruct((rows, heads * head_size), jnp.float32),
            jax.ShapeDtypeStruct((rows, head_size), jnp.float32),
        ],
        cost_estimate=pl.CostEstimate(
            flops=8 * heads * rows * positions * head_size,
            transcendentals=heads * rows * positions,
            bytes_accessed=10 * rows * heads * head_size,
        ),
        name="prefill",
    )(queries, keys, values, residual)


def scores_kernel(
    q_ref, old_ref, new_ref, own_ref, cursor_ref, p_old_ref, p_new_ref, p_own_ref, total_ref,
    *, key_heads, steps, blocks_per_head,
):
    heads, rows, head_size = q_ref.shape
    candidates = rows // steps
    factor = head_size ** (-0.5) * log2_e
    key_head = pl.program_id(0) // blocks_per_head
    old_count = old_ref.shape[0]
    new_count = new_ref.shape[0]
    own_count = own_ref.shape[1]
    q = q_ref[...].reshape(heads * rows, head_size)
    limit = jnp.concatenate([cursor_ref[...] * key_heads] * heads, axis=0)

    def far(keys, first, count):
        column = lax.broadcasted_iota(jnp.int32, (1, count), 1)
        column = jnp.where(lax.rem(column, key_heads) == key_head, column + first, 2**30)
        return jnp.where(column < limit, contract_last(q, keys), -jnp.inf)

    old = far(old_ref[...], 0, old_count)
    new = far(new_ref[...], old_count, new_count)
    row = lax.rem(lax.broadcasted_iota(jnp.int32, (heads * rows, own_count), 0), rows)
    column = lax.broadcasted_iota(jnp.int32, (heads * rows, own_count), 1)
    allowed = (lax.rem(row, candidates) == lax.rem(column, candidates)) & (column <= row)
    own = jnp.where(allowed, contract_last(q, own_ref[0]), -jnp.inf)
    top = jnp.maximum(
        jnp.maximum(jnp.max(old, axis=1, keepdims=True), jnp.max(new, axis=1, keepdims=True)),
        jnp.max(own, axis=1, keepdims=True),
    )
    old = jnp.exp2((old - top) * factor)
    new = jnp.exp2((new - top) * factor)
    own = jnp.exp2((own - top) * factor)
    total = (
        jnp.sum(old, axis=1, keepdims=True)
        + jnp.sum(new, axis=1, keepdims=True)
        + jnp.sum(own, axis=1, keepdims=True)
    )
    p_old_ref[...] = old.astype(jnp.bfloat16)
    p_new_ref[...] = new.astype(jnp.bfloat16)
    p_own_ref[...] = own.astype(jnp.bfloat16)
    total_ref[...] = jnp.broadcast_to(total, total_ref.shape)


def decode_scores(queries, old_keys, new_keys, own_keys, cursor, steps):
    heads, rows, head_size = queries.shape
    key_heads, own_count, _ = own_keys.shape
    old_count = old_keys.shape[0]
    new_count = new_keys.shape[0]
    per = heads // key_heads
    take = 4 if per % 4 == 0 else per
    whole = lambda i: (0, 0)
    return pl.pallas_call(
        functools.partial(
            scores_kernel, key_heads=key_heads, steps=steps, blocks_per_head=per // take
        ),
        grid=(heads // take,),
        in_specs=[
            pl.BlockSpec((take, rows, head_size), lambda i: (i, 0, 0)),
            pl.BlockSpec((old_count, head_size), whole),
            pl.BlockSpec((new_count, head_size), whole),
            pl.BlockSpec((1, own_count, head_size), lambda i: (i // (per // take), 0, 0)),
            pl.BlockSpec((rows, 1), whole),
        ],
        out_specs=[
            pl.BlockSpec((take * rows, old_count), lambda i: (i, 0)),
            pl.BlockSpec((take * rows, new_count), lambda i: (i, 0)),
            pl.BlockSpec((take * rows, own_count), lambda i: (i, 0)),
            pl.BlockSpec((take * rows, head_size), lambda i: (i, 0)),
        ],
        out_shape=[
            jax.ShapeDtypeStruct((heads * rows, old_count), jnp.bfloat16),
            jax.ShapeDtypeStruct((heads * rows, new_count), jnp.bfloat16),
            jax.ShapeDtypeStruct((heads * rows, own_count), jnp.bfloat16),
            jax.ShapeDtypeStruct((heads * rows, head_size), jnp.float32),
        ],
        cost_estimate=pl.CostEstimate(
            flops=8 * heads * rows * (old_count + new_count) * head_size,
            transcendentals=heads * rows * (old_count + new_count),
            bytes_accessed=2 * heads * rows * (old_count + new_count),
        ),
        name="decode_scores",
    )(queries, old_keys, new_keys, own_keys, cursor)


def mix_kernel(p_old_ref, p_own_ref, old_ref, own_ref, out_ref):
    out_ref[...] = jnp.dot(
        p_old_ref[...], old_ref[...], preferred_element_type=jnp.float32
    ) + jnp.dot(p_own_ref[...], own_ref[0], preferred_element_type=jnp.float32)


def decode_mix(p_old, p_own, old_values, own_values):
    rows, old_count = p_old.shape
    key_heads, own_count, head_size = own_values.shape
    block = rows // key_heads
    return pl.pallas_call(
        mix_kernel,
        grid=(key_heads,),
        in_specs=[
            pl.BlockSpec((block, old_count), lambda g: (g, 0)),
            pl.BlockSpec((block, own_count), lambda g: (g, 0)),
            pl.BlockSpec((old_count, head_size), lambda g: (0, 0)),
            pl.BlockSpec((1, own_count, head_size), lambda g: (g, 0, 0)),
        ],
        out_specs=pl.BlockSpec((block, head_size), lambda g: (g, 0)),
        out_shape=jax.ShapeDtypeStruct((rows, head_size), jnp.float32),
        cost_estimate=pl.CostEstimate(
            flops=4 * rows * old_count * head_size,
            transcendentals=0,
            bytes_accessed=2 * rows * old_count,
        ),
        name="decode_mix",
    )(p_old, p_own, old_values, own_values)


def finish_kernel(p_new_ref, new_ref, mixed_ref, total_ref, residual_ref, hidden_ref, squares_ref):
    rows = residual_ref.shape[0]
    head_size = mixed_ref.shape[1]
    heads = mixed_ref.shape[0] // rows
    mixed = mixed_ref[...] + jnp.dot(
        p_new_ref[...], new_ref[...], preferred_element_type=jnp.float32
    )
    mixed = mixed / total_ref[...]
    squares = jnp.zeros((rows, head_size), jnp.float32)
    for h in range(heads):
        lanes = slice(h * head_size, (h + 1) * head_size)
        hidden = mixed[h * rows : (h + 1) * rows] + residual_ref[:, lanes].astype(jnp.float32)
        hidden_ref[:, lanes] = hidden
        squares = squares + hidden * hidden
    squares = jnp.broadcast_to(jnp.sum(squares, axis=1, keepdims=True), (rows, 128))
    squares_ref[...] = jnp.transpose(squares)[:8]


def decode_finish(p_new, new_values, mixed, total, residual):
    rows, features = residual.shape
    return pl.pallas_call(
        finish_kernel,
        out_shape=[
            jax.ShapeDtypeStruct((rows, features), jnp.float32),
            jax.ShapeDtypeStruct((8, rows), jnp.float32),
        ],
        cost_estimate=pl.CostEstimate(
            flops=2 * p_new.shape[0] * p_new.shape[1] * new_values.shape[1],
            transcendentals=0,
            bytes_accessed=2 * p_new.shape[0] * p_new.shape[1],
        ),
        name="decode_finish",
    )(p_new, new_values, mixed, total, residual)


def local(
    prompt_keys,
    prompt_values,
    span_queries,
    span_keys,
    span_values,
    prefill_residual,
    decode_queries,
    decode_keys,
    decode_values,
    decode_residual,
    cursor,
    norm_gain,
):
    halfway = lax.axis_size("pair") // 2
    width = norm_gain.shape[0] * lax.axis_size("tp")
    old_keys = from_behind(prompt_keys, "pair", halfway)
    new_keys = from_behind(span_keys, "pair", halfway)
    old_values = from_behind(prompt_values, "pair", halfway)
    new_values = from_behind(span_values, "pair", halfway)
    gain_wide = norm_gain.astype(jnp.float32)

    def normed(hidden, squares):
        scale = lax.rsqrt(squares / width + epsilon)
        return (hidden * scale[..., None] * gain_wide).astype(jnp.bfloat16)

    head_major = lambda x: jnp.transpose(x, (1, 0, 2))
    keys = head_major(jnp.concatenate([prompt_keys[0], span_keys[0]], axis=0))
    values = head_major(jnp.concatenate([prompt_values[0], span_values[0]], axis=0))
    hidden, squares = prefill(head_major(span_queries[0]), keys, values, prefill_residual[0])
    prefill_normed = normed(hidden, lax.psum(jnp.sum(squares, axis=1), "tp"))

    steps, candidates, heads, head_size = decode_queries.shape[1:]
    rows = steps * candidates
    flat = lambda x: x[0].reshape(rows, x.shape[3], head_size)
    mixed_rows = lambda x: x[0].reshape(x.shape[1] * x.shape[2], head_size)
    own_values = head_major(flat(decode_values))
    limits = jnp.concatenate([cursor[0]] * steps)[:, None]
    p_old, p_new, p_own, total = decode_scores(
        head_major(flat(decode_queries)),
        mixed_rows(old_keys),
        mixed_rows(new_keys),
        head_major(flat(decode_keys)),
        limits,
        steps,
    )
    mixed = decode_mix(p_old, p_own, mixed_rows(old_values), own_values)
    hidden, squares = decode_finish(
        p_new, mixed_rows(new_values), mixed, total, decode_residual[0].reshape(rows, -1)
    )
    squares = sum_over(squares, "tp")
    decode_normed = normed(hidden, squares[0]).reshape(decode_residual.shape)
    handed_keys = jnp.concatenate([old_keys, new_keys], axis=1)
    handed_values = jnp.concatenate([old_values, new_values], axis=1)
    return (prefill_normed[None], handed_keys, handed_values, decode_normed)


def solution(mesh):
    whole = P(("groups", "pair"), None, "tp", None)
    step = P(("groups", "pair"), None, None, "tp", None)
    placed = (
        whole,
        whole,
        whole,
        whole,
        whole,
        P(("groups", "pair"), None, "tp"),
        step,
        step,
        step,
        P(("groups", "pair"), None, None, "tp"),
        P(("groups", "pair"), None),
        P("tp"),
    )
    return jax.shard_map(
        local,
        mesh=mesh,
        in_specs=placed,
        out_specs=(
            P(("groups", "pair"), None, "tp"),
            whole,
            whole,
            P(("groups", "pair"), None, None, "tp"),
        ),
        check_vma=False,
    )
```

```python
import functools

import jax
import jax.numpy as jnp
from jax import lax
from jax.experimental import pallas as pl
from jax.experimental.pallas import tpu as pltpu
from jax.sharding import PartitionSpec as P

epsilon = 1e-05
log2_e = 1.4426950408889634


def from_behind(value, axis, steps):
    count = lax.axis_size(axis)
    pairs = [(source, (source + steps) % count) for source in range(count)]
    return lax.ppermute(value, axis, pairs)


def sum_over(value, axis):
    count = lax.axis_size(axis)
    if count & (count - 1):
        return lax.psum(value, axis)
    step = count // 2
    while step:
        value = value + lax.ppermute(value, axis, [(i, i ^ step) for i in range(count)])
        step //= 2
    return value


def contract_last(a, b):
    return lax.dot_general(a, b, (((1,), (1,)), ((), ())), preferred_element_type=jnp.float32)


def prefill_kernel(q_ref, k_ref, v_ref, residual_ref, hidden_ref, squares_ref, *, block, past):
    rows = q_ref.shape[1]
    head_size = q_ref.shape[2]
    factor = head_size ** (-0.5) * log2_e

    @pl.when(pl.program_id(0) == 0)
    def _():
        squares_ref[...] = jnp.zeros_like(squares_ref)

    visible = lax.broadcasted_iota(jnp.int32, (block, block), 1) <= lax.broadcasted_iota(
        jnp.int32, (block, block), 0
    )
    for start in range(0, rows, block):
        here = slice(start, start + block)
        before = past + start
        q = q_ref[0, here]
        far = contract_last(q, k_ref[0, :before])
        near = contract_last(q, k_ref[0, before : before + block])
        near = jnp.where(visible, near, -jnp.inf)
        top = jnp.maximum(
            jnp.max(far, axis=1, keepdims=True), jnp.max(near, axis=1, keepdims=True)
        )
        far = jnp.exp2((far - top) * factor)
        near = jnp.exp2((near - top) * factor)
        total = jnp.sum(far, axis=1, keepdims=True) + jnp.sum(near, axis=1, keepdims=True)
        mixed = jnp.dot(
            far.astype(jnp.bfloat16), v_ref[0, :before], preferred_element_type=jnp.float32
        ) + jnp.dot(
            near.astype(jnp.bfloat16),
            v_ref[0, before : before + block],
            preferred_element_type=jnp.float32,
        )
        hidden = mixed / total + residual_ref[here].astype(jnp.float32)
        hidden_ref[here] = hidden
        squares_ref[here] = squares_ref[here] + hidden * hidden


def prefill(queries, keys, values, residual):
    heads, rows, head_size = queries.shape
    key_heads, positions, _ = keys.shape
    per = heads // key_heads
    block = 256 if rows % 256 == 0 else rows
    return pl.pallas_call(
        functools.partial(prefill_kernel, block=block, past=positions - rows),
        grid=(heads,),
        in_specs=[
            pl.BlockSpec((1, rows, head_size), lambda h: (h, 0, 0)),
            pl.BlockSpec((1, positions, head_size), lambda h: (h // per, 0, 0)),
            pl.BlockSpec((1, positions, head_size), lambda h: (h // per, 0, 0)),
            pl.BlockSpec((rows, head_size), lambda h: (0, h)),
        ],
        out_specs=[
            pl.BlockSpec((rows, head_size), lambda h: (0, h)),
            pl.BlockSpec((rows, head_size), lambda h: (0, 0)),
        ],
        out_shape=[
            jax.ShapeDtypeStruct((rows, heads * head_size), jnp.float32),
            jax.ShapeDtypeStruct((rows, head_size), jnp.float32),
        ],
        cost_estimate=pl.CostEstimate(
            flops=8 * heads * rows * positions * head_size,
            transcendentals=heads * rows * positions,
            bytes_accessed=10 * rows * heads * head_size,
        ),
        compiler_params=pltpu.CompilerParams(vmem_limit_bytes=32 << 20),
        name="prefill",
    )(queries, keys, values, residual)


def split_heads(rows_ref, wide_ref, out_ref, first):
    key_heads = out_ref.shape[0]
    count = rows_ref.shape[0]
    wide_ref[:count] = rows_ref[...].astype(jnp.float32)
    for g in range(key_heads):
        part = wide_ref[pl.ds(g, count // key_heads, stride=key_heads), :]
        out_ref[g, first : first + count // key_heads] = part.astype(out_ref.dtype)


def scores_kernel(
    q_ref, old_ref, new_ref, own_ref, cursor_ref,
    p_old_ref, p_new_ref, p_own_ref, inverse_ref, handed_ref,
    wide_ref, keys_ref, sems,
    *, steps,
):
    heads, rows, head_size = q_ref.shape
    key_heads, own_count, _ = own_ref.shape
    per = heads // key_heads
    take = 4 if per % 4 == 0 else per
    candidates = rows // steps
    factor = head_size ** (-0.5) * log2_e
    past = old_ref.shape[0]
    copies = [
        pltpu.make_async_copy(old_ref, handed_ref.at[:past], sems.at[0]),
        pltpu.make_async_copy(new_ref, handed_ref.at[past:], sems.at[1]),
    ]
    for copy in copies:
        copy.start()
    split_heads(old_ref, wide_ref, keys_ref, 0)
    split_heads(new_ref, wide_ref, keys_ref, past // key_heads)
    positions = keys_ref.shape[1]
    block = take * rows
    limit = jnp.concatenate([cursor_ref[...]] * take, axis=0)
    within = lax.broadcasted_iota(jnp.int32, (block, positions), 1) < limit
    row = lax.rem(lax.broadcasted_iota(jnp.int32, (block, own_count), 0), rows)
    column = lax.broadcasted_iota(jnp.int32, (block, own_count), 1)
    allowed = (lax.rem(row, candidates) == lax.rem(column, candidates)) & (column <= row)
    for first in range(0, heads, take):
        g = first // per
        here = slice(first * rows, first * rows + block)
        q = q_ref[first : first + take].reshape(block, head_size)
        far = jnp.where(within, contract_last(q, keys_ref[g]), -jnp.inf)
        own = jnp.where(allowed, contract_last(q, own_ref[g]), -jnp.inf)
        top = jnp.maximum(
            jnp.max(far, axis=1, keepdims=True), jnp.max(own, axis=1, keepdims=True)
        )
        far = jnp.exp2((far - top) * factor)
        own = jnp.exp2((own - top) * factor)
        total = jnp.sum(far, axis=1, keepdims=True) + jnp.sum(own, axis=1, keepdims=True)
        far = far.astype(jnp.bfloat16)
        p_old_ref[here] = far[:, : past // key_heads]
        p_new_ref[here] = far[:, past // key_heads :]
        p_own_ref[here] = own.astype(jnp.bfloat16)
        inverse_ref[here] = jnp.broadcast_to(1.0 / total, (block, head_size))
    for copy in copies:
        copy.wait()


HBM = pl.BlockSpec(memory_space=pltpu.HBM)
VMEM = pl.BlockSpec(memory_space=pltpu.VMEM)


def room(mib):
    return pltpu.CompilerParams(vmem_limit_bytes=mib << 20)


def decode_scores(queries, old_keys, new_keys, own_keys, cursor, steps):
    heads, rows, head_size = queries.shape
    key_heads, own_count, _ = own_keys.shape
    past = old_keys.shape[0] // key_heads
    span = new_keys.shape[0] // key_heads
    every = heads * rows
    return pl.pallas_call(
        functools.partial(scores_kernel, steps=steps),
        in_specs=[VMEM] * 5,
        out_specs=[VMEM] * 4 + [HBM],
        out_shape=[
            jax.ShapeDtypeStruct((every, past), jnp.bfloat16),
            jax.ShapeDtypeStruct((every, span), jnp.bfloat16),
            jax.ShapeDtypeStruct((every, own_count), jnp.bfloat16),
            jax.ShapeDtypeStruct((every, head_size), jnp.float32),
            jax.ShapeDtypeStruct((key_heads * (past + span), head_size), jnp.bfloat16),
        ],
        scratch_shapes=[
            pltpu.VMEM(old_keys.shape, jnp.float32),
            pltpu.VMEM((key_heads, past + span, head_size), jnp.bfloat16),
            pltpu.SemaphoreType.DMA((2,)),
        ],
        compiler_params=room(24),
        cost_estimate=pl.CostEstimate(
            flops=8 * every * (past + span) * head_size,
            transcendentals=every * (past + span),
            bytes_accessed=2 * every * (past + span),
        ),
        name="decode_scores",
    )(queries, old_keys, new_keys, own_keys, cursor)


def mix_kernel(
    p_old_ref, p_own_ref, inverse_ref, old_ref, own_ref, residual_ref,
    base_ref, handed_ref,
    wide_ref, values_ref, sem,
):
    rows = residual_ref.shape[0]
    key_heads, _, head_size = own_ref.shape
    heads = p_old_ref.shape[0] // rows
    per = heads // key_heads
    copy = pltpu.make_async_copy(old_ref, handed_ref.at[: old_ref.shape[0]], sem)
    copy.start()
    split_heads(old_ref, wide_ref, values_ref, 0)
    for g in range(key_heads):
        here = slice(g * per * rows, (g + 1) * per * rows)
        mixed = jnp.dot(p_old_ref[here], values_ref[g], preferred_element_type=jnp.float32)
        mixed += jnp.dot(p_own_ref[here], own_ref[g], preferred_element_type=jnp.float32)
        mixed *= inverse_ref[here]
        for h in range(per):
            lanes = slice((g * per + h) * head_size, (g * per + h + 1) * head_size)
            base_ref[:, lanes] = mixed[h * rows : (h + 1) * rows] + residual_ref[:, lanes].astype(
                jnp.float32
            )
    copy.wait()


def decode_mix(p_old, p_own, inverse, old_values, own_values, residual, positions):
    key_heads, _, head_size = own_values.shape
    return pl.pallas_call(
        mix_kernel,
        in_specs=[VMEM] * 6,
        out_specs=[VMEM, HBM],
        out_shape=[
            jax.ShapeDtypeStruct(residual.shape, jnp.float32),
            jax.ShapeDtypeStruct((key_heads * positions, head_size), jnp.bfloat16),
        ],
        scratch_shapes=[
            pltpu.VMEM(old_values.shape, jnp.float32),
            pltpu.VMEM(
                (key_heads, old_values.shape[0] // key_heads, head_size), jnp.bfloat16
            ),
            pltpu.SemaphoreType.DMA(()),
        ],
        compiler_params=room(16),
        cost_estimate=pl.CostEstimate(
            flops=4 * p_old.shape[0] * p_old.shape[1] * head_size,
            transcendentals=0,
            bytes_accessed=2 * p_old.shape[0] * p_old.shape[1],
        ),
        name="decode_mix",
    )(p_old, p_own, inverse, old_values, own_values, residual)


def finish_kernel(
    p_new_ref, inverse_ref, new_ref, base_ref, part_ref,
    hidden_ref, squares_ref, handed_ref,
    wide_ref, values_ref, sem,
):
    rows = base_ref.shape[0]
    key_heads, _, head_size = values_ref.shape
    heads = p_new_ref.shape[0] // rows
    per = heads // key_heads
    past = handed_ref.shape[0] - new_ref.shape[0]
    copy = pltpu.make_async_copy(new_ref, handed_ref.at[past:], sem)
    copy.start()
    split_heads(new_ref, wide_ref, values_ref, 0)
    squares = jnp.zeros((rows, head_size), jnp.float32)
    for g in range(key_heads):
        here = slice(g * per * rows, (g + 1) * per * rows)
        mixed = jnp.dot(p_new_ref[here], values_ref[g], preferred_element_type=jnp.float32)
        mixed *= inverse_ref[here]
        for h in range(per):
            lanes = slice((g * per + h) * head_size, (g * per + h + 1) * head_size)
            hidden = mixed[h * rows : (h + 1) * rows] + base_ref[:, lanes]
            hidden_ref[:, lanes] = hidden
            squares += hidden * hidden
    squares = jnp.broadcast_to(jnp.sum(squares, axis=1, keepdims=True), (rows, 128))
    squares_ref[...] = jnp.transpose(squares)[:8]
    copy.wait()


def decode_finish(p_new, inverse, new_values, base, part, key_heads):
    rows, features = base.shape
    head_size = new_values.shape[1]
    return pl.pallas_call(
        finish_kernel,
        in_specs=[VMEM] * 4 + [HBM],
        out_specs=[VMEM, VMEM, HBM],
        out_shape=[
            jax.ShapeDtypeStruct((rows, features), jnp.float32),
            jax.ShapeDtypeStruct((8, rows), jnp.float32),
            jax.ShapeDtypeStruct(part.shape, part.dtype),
        ],
        scratch_shapes=[
            pltpu.VMEM(new_values.shape, jnp.float32),
            pltpu.VMEM(
                (key_heads, new_values.shape[0] // key_heads, head_size), jnp.bfloat16
            ),
            pltpu.SemaphoreType.DMA(()),
        ],
        input_output_aliases={4: 2},
        compiler_params=room(8),
        cost_estimate=pl.CostEstimate(
            flops=2 * p_new.shape[0] * p_new.shape[1] * head_size,
            transcendentals=0,
            bytes_accessed=2 * p_new.shape[0] * p_new.shape[1],
        ),
        name="decode_finish",
    )(p_new, inverse, new_values, base, part)


def local(
    prompt_keys,
    prompt_values,
    span_queries,
    span_keys,
    span_values,
    prefill_residual,
    decode_queries,
    decode_keys,
    decode_values,
    decode_residual,
    cursor,
    norm_gain,
):
    halfway = lax.axis_size("pair") // 2
    keys_shape = (prompt_keys.shape[1] + span_keys.shape[1],) + prompt_keys.shape[2:]
    width = norm_gain.shape[0] * lax.axis_size("tp")
    old_keys = from_behind(prompt_keys, "pair", halfway)
    new_keys = from_behind(span_keys, "pair", halfway)
    old_values = from_behind(prompt_values, "pair", halfway)
    new_values = from_behind(span_values, "pair", halfway)
    gain_wide = norm_gain.astype(jnp.float32)

    def normed(hidden, squares):
        scale = lax.rsqrt(squares / width + epsilon)
        return (hidden * scale[..., None] * gain_wide).astype(jnp.bfloat16)

    head_major = lambda x: jnp.transpose(x, (1, 0, 2))
    keys = head_major(jnp.concatenate([prompt_keys[0], span_keys[0]], axis=0))
    values = head_major(jnp.concatenate([prompt_values[0], span_values[0]], axis=0))
    hidden, squares = prefill(head_major(span_queries[0]), keys, values, prefill_residual[0])
    prefill_normed = normed(hidden, lax.psum(jnp.sum(squares, axis=1), "tp"))

    steps, candidates, heads, head_size = decode_queries.shape[1:]
    rows = steps * candidates
    flat = lambda x: x[0].reshape(rows, x.shape[3], head_size)
    prefill_normed, decode_queries = lax.optimization_barrier((prefill_normed, decode_queries))
    mixed_rows = lambda x: x[0].reshape(x.shape[1] * x.shape[2], head_size)
    own_values = head_major(flat(decode_values))
    limits = jnp.concatenate([cursor[0]] * steps)[:, None]
    p_old, p_new, p_own, inverse, handed_keys = decode_scores(
        head_major(flat(decode_queries)),
        mixed_rows(old_keys),
        mixed_rows(new_keys),
        head_major(flat(decode_keys)),
        limits,
        steps,
    )
    positions, key_heads, _ = keys_shape
    base, part = decode_mix(
        p_old, p_own, inverse, mixed_rows(old_values), own_values,
        decode_residual[0].reshape(rows, -1), positions,
    )
    hidden, squares, handed_values = decode_finish(
        p_new, inverse, mixed_rows(new_values), base, part, key_heads
    )
    squares = sum_over(squares, "tp")
    decode_normed = normed(hidden, squares[0]).reshape(decode_residual.shape)
    whole = lambda x: x.reshape(1, positions, key_heads, head_size)
    return (prefill_normed[None], whole(handed_keys), whole(handed_values), decode_normed)


def solution(mesh):
    whole = P(("groups", "pair"), None, "tp", None)
    step = P(("groups", "pair"), None, None, "tp", None)
    placed = (
        whole,
        whole,
        whole,
        whole,
        whole,
        P(("groups", "pair"), None, "tp"),
        step,
        step,
        step,
        P(("groups", "pair"), None, None, "tp"),
        P(("groups", "pair"), None),
        P("tp"),
    )
    return jax.shard_map(
        local,
        mesh=mesh,
        in_specs=placed,
        out_specs=(
            P(("groups", "pair"), None, "tp"),
            whole,
            whole,
            P(("groups", "pair"), None, None, "tp"),
        ),
        check_vma=False,
    )
```

```python
import functools

import jax
import jax.numpy as jnp
from jax import lax
from jax.experimental import pallas as pl
from jax.experimental.pallas import tpu as pltpu
from jax.sharding import PartitionSpec as P

epsilon = 1e-05
log2_e = 1.4426950408889634


def from_behind(value, axis, steps):
    count = lax.axis_size(axis)
    pairs = [(source, (source + steps) % count) for source in range(count)]
    return lax.ppermute(value, axis, pairs)


def sum_over(value, axis):
    count = lax.axis_size(axis)
    if count & (count - 1):
        return lax.psum(value, axis)
    others = [
        lax.ppermute(value, axis, [(i, i ^ step) for i in range(count)])
        for step in (3, 2, 1)
    ]
    return functools.reduce(jnp.add, others, value)


def contract_last(a, b):
    return lax.dot_general(a, b, (((1,), (1,)), ((), ())), preferred_element_type=jnp.float32)


def prefill_kernel(q_ref, k_ref, v_ref, residual_ref, hidden_ref, squares_ref, *, block, past):
    rows = q_ref.shape[1]
    head_size = q_ref.shape[2]
    factor = head_size ** (-0.5) * log2_e

    @pl.when(pl.program_id(0) == 0)
    def _():
        squares_ref[...] = jnp.zeros_like(squares_ref)

    visible = lax.broadcasted_iota(jnp.int32, (block, block), 1) <= lax.broadcasted_iota(
        jnp.int32, (block, block), 0
    )
    for start in range(0, rows, block):
        here = slice(start, start + block)
        before = past + start
        q = q_ref[0, here]
        far = contract_last(q, k_ref[0, :before])
        near = contract_last(q, k_ref[0, before : before + block])
        near = jnp.where(visible, near, -jnp.inf)
        top = jnp.maximum(
            jnp.max(far, axis=1, keepdims=True), jnp.max(near, axis=1, keepdims=True)
        )
        far = jnp.exp2((far - top) * factor)
        near = jnp.exp2((near - top) * factor)
        total = jnp.sum(far, axis=1, keepdims=True) + jnp.sum(near, axis=1, keepdims=True)
        mixed = jnp.dot(
            far.astype(jnp.bfloat16), v_ref[0, :before], preferred_element_type=jnp.float32
        ) + jnp.dot(
            near.astype(jnp.bfloat16),
            v_ref[0, before : before + block],
            preferred_element_type=jnp.float32,
        )
        hidden = mixed / total + residual_ref[here].astype(jnp.float32)
        hidden_ref[here] = hidden
        squares_ref[here] = squares_ref[here] + hidden * hidden


def prefill(queries, keys, values, residual):
    heads, rows, head_size = queries.shape
    key_heads, positions, _ = keys.shape
    per = heads // key_heads
    block = 256 if rows % 256 == 0 else rows
    return pl.pallas_call(
        functools.partial(prefill_kernel, block=block, past=positions - rows),
        grid=(heads,),
        in_specs=[
            pl.BlockSpec((1, rows, head_size), lambda h: (h, 0, 0)),
            pl.BlockSpec((1, positions, head_size), lambda h: (h // per, 0, 0)),
            pl.BlockSpec((1, positions, head_size), lambda h: (h // per, 0, 0)),
            pl.BlockSpec((rows, head_size), lambda h: (0, h)),
        ],
        out_specs=[
            pl.BlockSpec((rows, head_size), lambda h: (0, h)),
            pl.BlockSpec((rows, head_size), lambda h: (0, 0)),
        ],
        out_shape=[
            jax.ShapeDtypeStruct((rows, heads * head_size), jnp.float32),
            jax.ShapeDtypeStruct((rows, head_size), jnp.float32),
        ],
        cost_estimate=pl.CostEstimate(
            flops=8 * heads * rows * positions * head_size,
            transcendentals=heads * rows * positions,
            bytes_accessed=10 * rows * heads * head_size,
        ),
        compiler_params=pltpu.CompilerParams(vmem_limit_bytes=32 << 20),
        name="prefill",
    )(queries, keys, values, residual)


def split_heads(rows_ref, wide_ref, out_ref, first):
    key_heads = out_ref.shape[0]
    count = rows_ref.shape[0]
    wide_ref[:count] = rows_ref[...].astype(jnp.float32)
    for g in range(key_heads):
        part = wide_ref[pl.ds(g, count // key_heads, stride=key_heads), :]
        out_ref[g, first : first + count // key_heads] = part.astype(out_ref.dtype)


def scores_kernel(
    q_ref, old_ref, new_ref, own_ref, cursor_ref,
    p_old_ref, p_new_ref, p_own_ref, inverse_ref, handed_ref,
    wide_ref, keys_ref, sems,
    *, steps,
):
    heads, rows, head_size = q_ref.shape
    key_heads, own_count, _ = own_ref.shape
    per = heads // key_heads
    take = 4 if per % 4 == 0 else per
    candidates = rows // steps
    factor = head_size ** (-0.5) * log2_e
    past = old_ref.shape[0]
    copies = [
        pltpu.make_async_copy(old_ref, handed_ref.at[:past], sems.at[0]),
        pltpu.make_async_copy(new_ref, handed_ref.at[past:], sems.at[1]),
    ]
    for copy in copies:
        copy.start()
    split_heads(old_ref, wide_ref, keys_ref, 0)
    split_heads(new_ref, wide_ref, keys_ref, past // key_heads)
    positions = keys_ref.shape[1]
    block = take * rows
    limit = jnp.concatenate([cursor_ref[...]] * take, axis=0)
    within = lax.broadcasted_iota(jnp.int32, (block, positions), 1) < limit
    row = lax.rem(lax.broadcasted_iota(jnp.int32, (block, own_count), 0), rows)
    column = lax.broadcasted_iota(jnp.int32, (block, own_count), 1)
    allowed = (lax.rem(row, candidates) == lax.rem(column, candidates)) & (column <= row)
    for first in range(0, heads, take):
        g = first // per
        here = slice(first * rows, first * rows + block)
        q = q_ref[first : first + take].reshape(block, head_size)
        far = jnp.where(within, contract_last(q, keys_ref[g]), -jnp.inf)
        own = jnp.where(allowed, contract_last(q, own_ref[g]), -jnp.inf)
        top = jnp.maximum(
            jnp.max(far, axis=1, keepdims=True), jnp.max(own, axis=1, keepdims=True)
        )
        far = jnp.exp2((far - top) * factor)
        own = jnp.exp2((own - top) * factor)
        total = jnp.sum(far, axis=1, keepdims=True) + jnp.sum(own, axis=1, keepdims=True)
        far = far.astype(jnp.bfloat16)
        p_old_ref[here] = far[:, : past // key_heads]
        p_new_ref[here] = far[:, past // key_heads :]
        p_own_ref[here] = own.astype(jnp.bfloat16)
        inverse_ref[here] = jnp.broadcast_to(1.0 / total, (block, head_size))
    for copy in copies:
        copy.wait()


HBM = pl.BlockSpec(memory_space=pltpu.HBM)
VMEM = pl.BlockSpec(memory_space=pltpu.VMEM)


def room(mib):
    return pltpu.CompilerParams(vmem_limit_bytes=mib << 20)


def decode_scores(queries, old_keys, new_keys, own_keys, cursor, steps):
    heads, rows, head_size = queries.shape
    key_heads, own_count, _ = own_keys.shape
    past = old_keys.shape[0] // key_heads
    span = new_keys.shape[0] // key_heads
    every = heads * rows
    return pl.pallas_call(
        functools.partial(scores_kernel, steps=steps),
        in_specs=[VMEM] * 5,
        out_specs=[VMEM] * 4 + [HBM],
        out_shape=[
            jax.ShapeDtypeStruct((every, past), jnp.bfloat16),
            jax.ShapeDtypeStruct((every, span), jnp.bfloat16),
            jax.ShapeDtypeStruct((every, own_count), jnp.bfloat16),
            jax.ShapeDtypeStruct((every, head_size), jnp.float32),
            jax.ShapeDtypeStruct((key_heads * (past + span), head_size), jnp.bfloat16),
        ],
        scratch_shapes=[
            pltpu.VMEM(old_keys.shape, jnp.float32),
            pltpu.VMEM((key_heads, past + span, head_size), jnp.bfloat16),
            pltpu.SemaphoreType.DMA((2,)),
        ],
        compiler_params=room(24),
        cost_estimate=pl.CostEstimate(
            flops=8 * every * (past + span) * head_size,
            transcendentals=every * (past + span),
            bytes_accessed=2 * every * (past + span),
        ),
        name="decode_scores",
    )(queries, old_keys, new_keys, own_keys, cursor)


def mix_kernel(
    p_old_ref, p_own_ref, inverse_ref, old_ref, own_ref, residual_ref,
    base_ref, handed_ref,
    wide_ref, values_ref, sem,
):
    rows = residual_ref.shape[0]
    key_heads, _, head_size = own_ref.shape
    heads = p_old_ref.shape[0] // rows
    per = heads // key_heads
    copy = pltpu.make_async_copy(old_ref, handed_ref.at[: old_ref.shape[0]], sem)
    copy.start()
    split_heads(old_ref, wide_ref, values_ref, 0)
    for g in range(key_heads):
        here = slice(g * per * rows, (g + 1) * per * rows)
        mixed = jnp.dot(p_old_ref[here], values_ref[g], preferred_element_type=jnp.float32)
        mixed += jnp.dot(p_own_ref[here], own_ref[g], preferred_element_type=jnp.float32)
        mixed *= inverse_ref[here]
        for h in range(per):
            lanes = slice((g * per + h) * head_size, (g * per + h + 1) * head_size)
            base_ref[:, lanes] = mixed[h * rows : (h + 1) * rows] + residual_ref[:, lanes].astype(
                jnp.float32
            )
    copy.wait()


def decode_mix(p_old, p_own, inverse, old_values, own_values, residual, positions):
    key_heads, _, head_size = own_values.shape
    return pl.pallas_call(
        mix_kernel,
        in_specs=[VMEM] * 6,
        out_specs=[VMEM, HBM],
        out_shape=[
            jax.ShapeDtypeStruct(residual.shape, jnp.float32),
            jax.ShapeDtypeStruct((key_heads * positions, head_size), jnp.bfloat16),
        ],
        scratch_shapes=[
            pltpu.VMEM(old_values.shape, jnp.float32),
            pltpu.VMEM(
                (key_heads, old_values.shape[0] // key_heads, head_size), jnp.bfloat16
            ),
            pltpu.SemaphoreType.DMA(()),
        ],
        compiler_params=room(16),
        cost_estimate=pl.CostEstimate(
            flops=4 * p_old.shape[0] * p_old.shape[1] * head_size,
            transcendentals=0,
            bytes_accessed=2 * p_old.shape[0] * p_old.shape[1],
        ),
        name="decode_mix",
    )(p_old, p_own, inverse, old_values, own_values, residual)


def finish_kernel(
    p_new_ref, inverse_ref, new_ref, base_ref,
    hidden_ref, squares_ref,
    wide_ref, values_ref,
):
    rows = base_ref.shape[0]
    key_heads, _, head_size = values_ref.shape
    heads = p_new_ref.shape[0] // rows
    per = heads // key_heads
    split_heads(new_ref, wide_ref, values_ref, 0)
    squares = jnp.zeros((rows, head_size), jnp.float32)
    for g in range(key_heads):
        here = slice(g * per * rows, (g + 1) * per * rows)
        mixed = jnp.dot(p_new_ref[here], values_ref[g], preferred_element_type=jnp.float32)
        mixed *= inverse_ref[here]
        for h in range(per):
            lanes = slice((g * per + h) * head_size, (g * per + h + 1) * head_size)
            hidden = mixed[h * rows : (h + 1) * rows] + base_ref[:, lanes]
            hidden_ref[:, lanes] = hidden
            squares += hidden * hidden
    squares = jnp.broadcast_to(jnp.sum(squares, axis=1, keepdims=True), (rows, 128))
    squares_ref[...] = jnp.transpose(squares)[:8]


def decode_finish(p_new, inverse, new_values, base, key_heads):
    rows, features = base.shape
    head_size = new_values.shape[1]
    return pl.pallas_call(
        finish_kernel,
        in_specs=[VMEM] * 4,
        out_specs=[VMEM] * 2,
        out_shape=[
            jax.ShapeDtypeStruct((rows, features), jnp.float32),
            jax.ShapeDtypeStruct((8, rows), jnp.float32),
        ],
        scratch_shapes=[
            pltpu.VMEM(new_values.shape, jnp.float32),
            pltpu.VMEM(
                (key_heads, new_values.shape[0] // key_heads, head_size), jnp.bfloat16
            ),
        ],
        compiler_params=room(8),
        cost_estimate=pl.CostEstimate(
            flops=2 * p_new.shape[0] * p_new.shape[1] * head_size,
            transcendentals=0,
            bytes_accessed=2 * p_new.shape[0] * p_new.shape[1],
        ),
        name="decode_finish",
    )(p_new, inverse, new_values, base)


def append_kernel(new_ref, part_ref, after_ref, handed_ref, sem):
    copy = pltpu.make_async_copy(
        new_ref, handed_ref.at[handed_ref.shape[0] - new_ref.shape[0] :], sem
    )
    copy.start()
    copy.wait()


def append(part, new, after):
    return pl.pallas_call(
        append_kernel,
        in_specs=[VMEM, HBM, VMEM],
        out_specs=HBM,
        out_shape=jax.ShapeDtypeStruct(part.shape, part.dtype),
        scratch_shapes=[pltpu.SemaphoreType.DMA(())],
        input_output_aliases={1: 0},
        compiler_params=room(2),
        cost_estimate=pl.CostEstimate(
            flops=1000000, transcendentals=0, bytes_accessed=4 * new.size
        ),
        name="append",
    )(new, part, after)


def local(
    prompt_keys,
    prompt_values,
    span_queries,
    span_keys,
    span_values,
    prefill_residual,
    decode_queries,
    decode_keys,
    decode_values,
    decode_residual,
    cursor,
    norm_gain,
):
    halfway = lax.axis_size("pair") // 2
    keys_shape = (prompt_keys.shape[1] + span_keys.shape[1],) + prompt_keys.shape[2:]
    width = norm_gain.shape[0] * lax.axis_size("tp")
    old_keys = from_behind(prompt_keys, "pair", halfway)
    new_keys = from_behind(span_keys, "pair", halfway)
    old_values = from_behind(prompt_values, "pair", halfway)
    new_values = from_behind(span_values, "pair", halfway)
    gain_wide = norm_gain.astype(jnp.float32)

    def normed(hidden, squares):
        scale = lax.rsqrt(squares / width + epsilon)
        return (hidden * scale[..., None] * gain_wide).astype(jnp.bfloat16)

    head_major = lambda x: jnp.transpose(x, (1, 0, 2))
    keys = head_major(jnp.concatenate([prompt_keys[0], span_keys[0]], axis=0))
    values = head_major(jnp.concatenate([prompt_values[0], span_values[0]], axis=0))
    hidden, squares = prefill(head_major(span_queries[0]), keys, values, prefill_residual[0])
    prefill_normed = normed(hidden, lax.psum(jnp.sum(squares, axis=1), "tp"))

    steps, candidates, heads, head_size = decode_queries.shape[1:]
    rows = steps * candidates
    flat = lambda x: x[0].reshape(rows, x.shape[3], head_size)
    prefill_normed, decode_queries = lax.optimization_barrier((prefill_normed, decode_queries))
    mixed_rows = lambda x: x[0].reshape(x.shape[1] * x.shape[2], head_size)
    own_values = head_major(flat(decode_values))
    limits = jnp.concatenate([cursor[0]] * steps)[:, None]
    p_old, p_new, p_own, inverse, handed_keys = decode_scores(
        head_major(flat(decode_queries)),
        mixed_rows(old_keys),
        mixed_rows(new_keys),
        head_major(flat(decode_keys)),
        limits,
        steps,
    )
    positions, key_heads, _ = keys_shape
    base, part = decode_mix(
        p_old, p_own, inverse, mixed_rows(old_values), own_values,
        decode_residual[0].reshape(rows, -1), positions,
    )
    new_rows = mixed_rows(new_values)
    hidden, squares = decode_finish(p_new, inverse, new_rows, base, key_heads)
    handed_values = append(part, new_rows, squares)
    squares = sum_over(squares, "tp")
    decode_normed = normed(hidden, squares[0]).reshape(decode_residual.shape)
    whole = lambda x: x.reshape(1, positions, key_heads, head_size)
    return (prefill_normed[None], whole(handed_keys), whole(handed_values), decode_normed)


def solution(mesh):
    whole = P(("groups", "pair"), None, "tp", None)
    step = P(("groups", "pair"), None, None, "tp", None)
    placed = (
        whole,
        whole,
        whole,
        whole,
        whole,
        P(("groups", "pair"), None, "tp"),
        step,
        step,
        step,
        P(("groups", "pair"), None, None, "tp"),
        P(("groups", "pair"), None),
        P("tp"),
    )
    return jax.shard_map(
        local,
        mesh=mesh,
        in_specs=placed,
        out_specs=(
            P(("groups", "pair"), None, "tp"),
            whole,
            whole,
            P(("groups", "pair"), None, None, "tp"),
        ),
        check_vma=False,
    )
```

```python
import functools

import jax
import jax.numpy as jnp
from jax import lax
from jax.experimental import pallas as pl
from jax.experimental.pallas import tpu as pltpu
from jax.sharding import PartitionSpec as P

epsilon = 1e-05
log2_e = 1.4426950408889634
late_rows = 128


def from_behind(value, axis, steps):
    count = lax.axis_size(axis)
    pairs = [(source, (source + steps) % count) for source in range(count)]
    return lax.ppermute(value, axis, pairs)


def sum_over(value, axis):
    count = lax.axis_size(axis)
    if count & (count - 1):
        return lax.psum(value, axis)
    others = [
        lax.ppermute(value, axis, [(i, i ^ step) for i in range(count)])
        for step in (3, 2, 1)
    ]
    return functools.reduce(jnp.add, others, value)


def contract_last(a, b):
    return lax.dot_general(a, b, (((1,), (1,)), ((), ())), preferred_element_type=jnp.float32)


def prefill_kernel(q_ref, k_ref, v_ref, residual_ref, hidden_ref, squares_ref, *, block, past):
    rows = q_ref.shape[1]
    head_size = q_ref.shape[2]
    factor = head_size ** (-0.5) * log2_e

    @pl.when(pl.program_id(0) == 0)
    def _():
        squares_ref[...] = jnp.zeros_like(squares_ref)

    visible = lax.broadcasted_iota(jnp.int32, (block, block), 1) <= lax.broadcasted_iota(
        jnp.int32, (block, block), 0
    )
    for start in range(0, rows, block):
        here = slice(start, start + block)
        before = past + start
        q = q_ref[0, here]
        far = contract_last(q, k_ref[0, :before])
        near = contract_last(q, k_ref[0, before : before + block])
        near = jnp.where(visible, near, -jnp.inf)
        top = jnp.maximum(
            jnp.max(far, axis=1, keepdims=True), jnp.max(near, axis=1, keepdims=True)
        )
        far = jnp.exp2((far - top) * factor)
        near = jnp.exp2((near - top) * factor)
        total = jnp.sum(far, axis=1, keepdims=True) + jnp.sum(near, axis=1, keepdims=True)
        mixed = jnp.dot(
            far.astype(jnp.bfloat16), v_ref[0, :before], preferred_element_type=jnp.float32
        ) + jnp.dot(
            near.astype(jnp.bfloat16),
            v_ref[0, before : before + block],
            preferred_element_type=jnp.float32,
        )
        hidden = mixed / total + residual_ref[here].astype(jnp.float32)
        hidden_ref[here] = hidden
        squares_ref[here] = squares_ref[here] + hidden * hidden


def prefill(queries, keys, values, residual):
    heads, rows, head_size = queries.shape
    key_heads, positions, _ = keys.shape
    per = heads // key_heads
    block = 256 if rows % 256 == 0 else rows
    return pl.pallas_call(
        functools.partial(prefill_kernel, block=block, past=positions - rows),
        grid=(heads,),
        in_specs=[
            pl.BlockSpec((1, rows, head_size), lambda h: (h, 0, 0)),
            pl.BlockSpec((1, positions, head_size), lambda h: (h // per, 0, 0)),
            pl.BlockSpec((1, positions, head_size), lambda h: (h // per, 0, 0)),
            pl.BlockSpec((rows, head_size), lambda h: (0, h)),
        ],
        out_specs=[
            pl.BlockSpec((rows, head_size), lambda h: (0, h)),
            pl.BlockSpec((rows, head_size), lambda h: (0, 0)),
        ],
        out_shape=[
            jax.ShapeDtypeStruct((rows, heads * head_size), jnp.float32),
            jax.ShapeDtypeStruct((rows, head_size), jnp.float32),
        ],
        cost_estimate=pl.CostEstimate(
            flops=8 * heads * rows * positions * head_size,
            transcendentals=heads * rows * positions,
            bytes_accessed=10 * rows * heads * head_size,
        ),
        compiler_params=pltpu.CompilerParams(vmem_limit_bytes=32 << 20),
        name="prefill",
    )(queries, keys, values, residual)


def split_heads(rows_ref, wide_ref, out_ref, first):
    key_heads = out_ref.shape[0]
    count = rows_ref.shape[0]
    wide_ref[:count] = rows_ref[...].astype(jnp.float32)
    for g in range(key_heads):
        part = wide_ref[pl.ds(g, count // key_heads, stride=key_heads), :]
        out_ref[g, first : first + count // key_heads] = part.astype(out_ref.dtype)


def scores_kernel(
    q_ref, old_ref, new_ref, own_ref, cursor_ref,
    p_old_ref, p_new_ref, p_own_ref, inverse_ref, handed_ref,
    wide_ref, keys_ref, sems,
    *, steps, early, late,
):
    heads, rows, head_size = q_ref.shape
    key_heads, own_count, _ = own_ref.shape
    per = heads // key_heads
    take = 4 if per % 4 == 0 else per
    candidates = rows // steps
    factor = head_size ** (-0.5) * log2_e
    past = old_ref.shape[0]
    copies = [
        pltpu.make_async_copy(old_ref, handed_ref.at[:past], sems.at[0]),
        pltpu.make_async_copy(new_ref, handed_ref.at[past:], sems.at[1]),
    ]
    for copy in copies:
        copy.start()
    split_heads(old_ref, wide_ref, keys_ref, 0)
    split_heads(new_ref, wide_ref, keys_ref, past // key_heads)
    positions = keys_ref.shape[1]
    block = take * rows
    limit = jnp.concatenate([cursor_ref[...]] * take, axis=0)
    within = lax.broadcasted_iota(jnp.int32, (block, positions), 1) < limit
    row = lax.rem(lax.broadcasted_iota(jnp.int32, (block, own_count), 0), rows)
    column = lax.broadcasted_iota(jnp.int32, (block, own_count), 1)
    allowed = (lax.rem(row, candidates) == lax.rem(column, candidates)) & (column <= row)
    for first in range(0, heads, take):
        g = first // per
        here = slice(first * rows, first * rows + block)
        q = q_ref[first : first + take].reshape(block, head_size)
        far = jnp.where(within, contract_last(q, keys_ref[g]), -jnp.inf)
        own = jnp.where(allowed, contract_last(q, own_ref[g]), -jnp.inf)
        top = jnp.maximum(
            jnp.max(far, axis=1, keepdims=True), jnp.max(own, axis=1, keepdims=True)
        )
        far = jnp.exp2((far - top) * factor)
        own = jnp.exp2((own - top) * factor)
        total = jnp.sum(far, axis=1, keepdims=True) + jnp.sum(own, axis=1, keepdims=True)
        far = far.astype(jnp.bfloat16)
        for p_ref, chunks in ((p_old_ref, early), (p_new_ref, late)):
            first_column = 0
            for start, stop in chunks:
                columns = slice(first_column, first_column + stop - start)
                p_ref[here, columns] = far[:, start:stop]
                first_column = columns.stop
        p_own_ref[here] = own.astype(jnp.bfloat16)
        inverse_ref[here] = jnp.broadcast_to(1.0 / total, (block, head_size))
    for copy in copies:
        copy.wait()


HBM = pl.BlockSpec(memory_space=pltpu.HBM)
VMEM = pl.BlockSpec(memory_space=pltpu.VMEM)


def length(chunks):
    return sum(stop - start for start, stop in chunks)


def copies_of(refs, chunks, handed_ref, sems):
    copies = []
    for i, (ref, (start, stop)) in enumerate(zip(refs, chunks)):
        per = ref.shape[0] // (stop - start)
        copies.append(
            pltpu.make_async_copy(ref, handed_ref.at[start * per : stop * per], sems.at[i])
        )
        copies[-1].start()
    return copies


def split_all(refs, chunks, wide_ref, out_ref):
    first = 0
    for ref, (start, stop) in zip(refs, chunks):
        split_heads(ref, wide_ref, out_ref, first)
        first += stop - start


def room(mib):
    return pltpu.CompilerParams(vmem_limit_bytes=mib << 20)


def decode_scores(queries, old_keys, new_keys, own_keys, cursor, steps, early, late):
    heads, rows, head_size = queries.shape
    key_heads, own_count, _ = own_keys.shape
    past = old_keys.shape[0] // key_heads
    span = new_keys.shape[0] // key_heads
    every = heads * rows
    return pl.pallas_call(
        functools.partial(scores_kernel, steps=steps, early=early, late=late),
        in_specs=[VMEM] * 5,
        out_specs=[VMEM] * 4 + [HBM],
        out_shape=[
            jax.ShapeDtypeStruct((every, length(early)), jnp.bfloat16),
            jax.ShapeDtypeStruct((every, length(late)), jnp.bfloat16),
            jax.ShapeDtypeStruct((every, own_count), jnp.bfloat16),
            jax.ShapeDtypeStruct((every, head_size), jnp.float32),
            jax.ShapeDtypeStruct((key_heads * (past + span), head_size), jnp.bfloat16),
        ],
        scratch_shapes=[
            pltpu.VMEM(old_keys.shape, jnp.float32),
            pltpu.VMEM((key_heads, past + span, head_size), jnp.bfloat16),
            pltpu.SemaphoreType.DMA((2,)),
        ],
        compiler_params=room(24),
        cost_estimate=pl.CostEstimate(
            flops=8 * every * (past + span) * head_size,
            transcendentals=every * (past + span),
            bytes_accessed=2 * every * (past + span),
        ),
        name="decode_scores",
    )(queries, old_keys, new_keys, own_keys, cursor)


def mix_kernel(*refs, early):
    p_old_ref, p_own_ref, inverse_ref, own_ref, residual_ref = refs[:5]
    chunk_refs = refs[5 : 5 + len(early)]
    base_ref, handed_ref, wide_ref, values_ref, sems = refs[5 + len(early) :]
    rows = residual_ref.shape[0]
    key_heads, _, head_size = own_ref.shape
    heads = p_old_ref.shape[0] // rows
    per = heads // key_heads
    copies = copies_of(chunk_refs, early, handed_ref, sems)
    split_all(chunk_refs, early, wide_ref, values_ref)
    for g in range(key_heads):
        here = slice(g * per * rows, (g + 1) * per * rows)
        mixed = jnp.dot(p_old_ref[here], values_ref[g], preferred_element_type=jnp.float32)
        mixed += jnp.dot(p_own_ref[here], own_ref[g], preferred_element_type=jnp.float32)
        mixed *= inverse_ref[here]
        for h in range(per):
            lanes = slice((g * per + h) * head_size, (g * per + h + 1) * head_size)
            base_ref[:, lanes] = mixed[h * rows : (h + 1) * rows] + residual_ref[:, lanes].astype(
                jnp.float32
            )
    for copy in copies:
        copy.wait()


def decode_mix(p_old, p_own, inverse, own_values, residual, chunk_values, early, positions):
    key_heads, _, head_size = own_values.shape
    most = max(x.shape[0] for x in chunk_values)
    return pl.pallas_call(
        functools.partial(mix_kernel, early=early),
        in_specs=[VMEM] * (5 + len(early)),
        out_specs=[VMEM, HBM],
        out_shape=[
            jax.ShapeDtypeStruct(residual.shape, jnp.float32),
            jax.ShapeDtypeStruct((key_heads * positions, head_size), jnp.bfloat16),
        ],
        scratch_shapes=[
            pltpu.VMEM((most, head_size), jnp.float32),
            pltpu.VMEM((key_heads, length(early), head_size), jnp.bfloat16),
            pltpu.SemaphoreType.DMA((len(early),)),
        ],
        compiler_params=room(16),
        cost_estimate=pl.CostEstimate(
            flops=4 * p_old.shape[0] * p_old.shape[1] * head_size,
            transcendentals=0,
            bytes_accessed=2 * p_old.shape[0] * p_old.shape[1],
        ),
        name="decode_mix",
    )(p_old, p_own, inverse, own_values, residual, *chunk_values)


def finish_kernel(*refs, late):
    p_new_ref, inverse_ref, base_ref = refs[:3]
    chunk_refs = refs[3 : 3 + len(late)]
    hidden_ref, squares_ref, wide_ref, values_ref = refs[3 + len(late) :]
    rows = base_ref.shape[0]
    key_heads, _, head_size = values_ref.shape
    heads = p_new_ref.shape[0] // rows
    per = heads // key_heads
    split_all(chunk_refs, late, wide_ref, values_ref)
    squares = jnp.zeros((rows, head_size), jnp.float32)
    for g in range(key_heads):
        here = slice(g * per * rows, (g + 1) * per * rows)
        mixed = jnp.dot(p_new_ref[here], values_ref[g], preferred_element_type=jnp.float32)
        mixed *= inverse_ref[here]
        for h in range(per):
            lanes = slice((g * per + h) * head_size, (g * per + h + 1) * head_size)
            hidden = mixed[h * rows : (h + 1) * rows] + base_ref[:, lanes]
            hidden_ref[:, lanes] = hidden
            squares += hidden * hidden
    squares = jnp.broadcast_to(jnp.sum(squares, axis=1, keepdims=True), (rows, 128))
    squares_ref[...] = jnp.transpose(squares)[:8]


def decode_finish(p_new, inverse, base, chunk_values, late):
    rows, features = base.shape
    most, head_size = max(x.shape for x in chunk_values)
    key_heads = sum(x.shape[0] for x in chunk_values) // length(late)
    return pl.pallas_call(
        functools.partial(finish_kernel, late=late),
        in_specs=[VMEM] * (3 + len(late)),
        out_specs=[VMEM] * 2,
        out_shape=[
            jax.ShapeDtypeStruct((rows, features), jnp.float32),
            jax.ShapeDtypeStruct((8, rows), jnp.float32),
        ],
        scratch_shapes=[
            pltpu.VMEM((most, head_size), jnp.float32),
            pltpu.VMEM((key_heads, length(late), head_size), jnp.bfloat16),
        ],
        compiler_params=room(8),
        cost_estimate=pl.CostEstimate(
            flops=2 * p_new.shape[0] * p_new.shape[1] * head_size,
            transcendentals=0,
            bytes_accessed=2 * p_new.shape[0] * p_new.shape[1],
        ),
        name="decode_finish",
    )(p_new, inverse, base, *chunk_values)


def append_kernel(*refs, late):
    *chunk_refs, _, _, handed_ref, sems = refs
    for copy in copies_of(chunk_refs, late, handed_ref, sems):
        copy.wait()


def append(part, chunk_values, late, after):
    return pl.pallas_call(
        functools.partial(append_kernel, late=late),
        in_specs=[VMEM] * len(late) + [HBM, VMEM],
        out_specs=HBM,
        out_shape=jax.ShapeDtypeStruct(part.shape, part.dtype),
        scratch_shapes=[pltpu.SemaphoreType.DMA((len(late),))],
        input_output_aliases={len(late): 0},
        compiler_params=room(2),
        cost_estimate=pl.CostEstimate(
            flops=1000000,
            transcendentals=0,
            bytes_accessed=4 * sum(x.size for x in chunk_values),
        ),
        name="append",
    )(*chunk_values, part, after)


def local(
    prompt_keys,
    prompt_values,
    span_queries,
    span_keys,
    span_values,
    prefill_residual,
    decode_queries,
    decode_keys,
    decode_values,
    decode_residual,
    cursor,
    norm_gain,
):
    halfway = lax.axis_size("pair") // 2
    keys_shape = (prompt_keys.shape[1] + span_keys.shape[1],) + prompt_keys.shape[2:]
    width = norm_gain.shape[0] * lax.axis_size("tp")
    old_keys = from_behind(prompt_keys, "pair", halfway)
    new_keys = from_behind(span_keys, "pair", halfway)
    past, span = prompt_values.shape[1], span_values.shape[1]
    late_past, late_span = min(late_rows, past), min(late_rows, span)
    early = ((0, past - late_past), (past, past + span - late_span))
    late = ((past - late_past, past), (past + span - late_span, past + span))
    early, late = [[(a, b) for a, b in chunks if b > a] for chunks in (early, late)]

    def received(chunk):
        start, stop = chunk
        if start < past:
            rows = prompt_values[:, start:stop]
        else:
            rows = span_values[:, start - past : stop - past]
        rows = from_behind(rows, "pair", halfway)[0]
        return rows.reshape(-1, rows.shape[-1])

    early_values = [received(chunk) for chunk in early]
    late_values = [received(chunk) for chunk in late]
    gain_wide = norm_gain.astype(jnp.float32)

    def normed(hidden, squares):
        scale = lax.rsqrt(squares / width + epsilon)
        return (hidden * scale[..., None] * gain_wide).astype(jnp.bfloat16)

    head_major = lambda x: jnp.transpose(x, (1, 0, 2))
    keys = head_major(jnp.concatenate([prompt_keys[0], span_keys[0]], axis=0))
    values = head_major(jnp.concatenate([prompt_values[0], span_values[0]], axis=0))
    hidden, squares = prefill(head_major(span_queries[0]), keys, values, prefill_residual[0])
    prefill_normed = normed(hidden, lax.psum(jnp.sum(squares, axis=1), "tp"))

    steps, candidates, heads, head_size = decode_queries.shape[1:]
    rows = steps * candidates
    flat = lambda x: x[0].reshape(rows, x.shape[3], head_size)
    prefill_normed, decode_queries = lax.optimization_barrier((prefill_normed, decode_queries))
    mixed_rows = lambda x: x[0].reshape(x.shape[1] * x.shape[2], head_size)
    own_values = head_major(flat(decode_values))
    limits = jnp.concatenate([cursor[0]] * steps)[:, None]
    p_old, p_new, p_own, inverse, handed_keys = decode_scores(
        head_major(flat(decode_queries)),
        mixed_rows(old_keys),
        mixed_rows(new_keys),
        head_major(flat(decode_keys)),
        limits,
        steps,
        early,
        late,
    )
    positions, key_heads, _ = keys_shape
    base, part = decode_mix(
        p_old, p_own, inverse, own_values, decode_residual[0].reshape(rows, -1),
        early_values, early, positions,
    )
    hidden, squares = decode_finish(p_new, inverse, base, late_values, late)
    handed_values = append(part, late_values, late, squares)
    squares = sum_over(squares, "tp")
    decode_normed = normed(hidden, squares[0]).reshape(decode_residual.shape)
    whole = lambda x: x.reshape(1, positions, key_heads, head_size)
    return (prefill_normed[None], whole(handed_keys), whole(handed_values), decode_normed)


def solution(mesh):
    whole = P(("groups", "pair"), None, "tp", None)
    step = P(("groups", "pair"), None, None, "tp", None)
    placed = (
        whole,
        whole,
        whole,
        whole,
        whole,
        P(("groups", "pair"), None, "tp"),
        step,
        step,
        step,
        P(("groups", "pair"), None, None, "tp"),
        P(("groups", "pair"), None),
        P("tp"),
    )
    return jax.shard_map(
        local,
        mesh=mesh,
        in_specs=placed,
        out_specs=(
            P(("groups", "pair"), None, "tp"),
            whole,
            whole,
            P(("groups", "pair"), None, None, "tp"),
        ),
        check_vma=False,
    )
```

```python
import functools

import jax
import jax.numpy as jnp
from jax import lax
from jax.experimental import pallas as pl
from jax.experimental.pallas import tpu as pltpu
from jax.sharding import PartitionSpec as P

epsilon = 1e-05
log2_e = 1.4426950408889634
late_rows = 128


def from_behind(value, axis, steps):
    count = lax.axis_size(axis)
    pairs = [(source, (source + steps) % count) for source in range(count)]
    return lax.ppermute(value, axis, pairs)


def sum_over(value, axis):
    count = lax.axis_size(axis)
    if count & (count - 1):
        return lax.psum(value, axis)
    others = [
        lax.ppermute(value, axis, [(i, i ^ step) for i in range(count)])
        for step in range(count - 1, 0, -1)
    ]
    return functools.reduce(jnp.add, others, value)


def contract_last(a, b):
    return lax.dot_general(a, b, (((1,), (1,)), ((), ())), preferred_element_type=jnp.float32)


def prefill_kernel(q_ref, k_ref, v_ref, residual_ref, hidden_ref, squares_ref, *, block, past):
    rows = q_ref.shape[1]
    head_size = q_ref.shape[2]
    factor = head_size ** (-0.5) * log2_e

    @pl.when(pl.program_id(0) == 0)
    def _():
        squares_ref[...] = jnp.zeros_like(squares_ref)

    visible = lax.broadcasted_iota(jnp.int32, (block, block), 1) <= lax.broadcasted_iota(
        jnp.int32, (block, block), 0
    )
    for start in range(0, rows, block):
        here = slice(start, start + block)
        before = past + start
        q = q_ref[0, here]
        far = contract_last(q, k_ref[0, :before])
        near = contract_last(q, k_ref[0, before : before + block])
        near = jnp.where(visible, near, -jnp.inf)
        top = jnp.maximum(
            jnp.max(far, axis=1, keepdims=True), jnp.max(near, axis=1, keepdims=True)
        )
        far = jnp.exp2((far - top) * factor)
        near = jnp.exp2((near - top) * factor)
        total = jnp.sum(far, axis=1, keepdims=True) + jnp.sum(near, axis=1, keepdims=True)
        mixed = jnp.dot(
            far.astype(jnp.bfloat16), v_ref[0, :before], preferred_element_type=jnp.float32
        ) + jnp.dot(
            near.astype(jnp.bfloat16),
            v_ref[0, before : before + block],
            preferred_element_type=jnp.float32,
        )
        hidden = mixed / total + residual_ref[here].astype(jnp.float32)
        hidden_ref[here] = hidden
        squares_ref[here] = squares_ref[here] + hidden * hidden


def prefill(queries, keys, values, residual):
    heads, rows, head_size = queries.shape
    key_heads, positions, _ = keys.shape
    per = heads // key_heads
    block = 256 if rows % 256 == 0 else rows
    return pl.pallas_call(
        functools.partial(prefill_kernel, block=block, past=positions - rows),
        grid=(heads,),
        in_specs=[
            pl.BlockSpec((1, rows, head_size), lambda h: (h, 0, 0)),
            pl.BlockSpec((1, positions, head_size), lambda h: (h // per, 0, 0)),
            pl.BlockSpec((1, positions, head_size), lambda h: (h // per, 0, 0)),
            pl.BlockSpec((rows, head_size), lambda h: (0, h)),
        ],
        out_specs=[
            pl.BlockSpec((rows, head_size), lambda h: (0, h)),
            pl.BlockSpec((rows, head_size), lambda h: (0, 0)),
        ],
        out_shape=[
            jax.ShapeDtypeStruct((rows, heads * head_size), jnp.float32),
            jax.ShapeDtypeStruct((rows, head_size), jnp.float32),
        ],
        cost_estimate=pl.CostEstimate(
            flops=8 * heads * rows * positions * head_size,
            transcendentals=heads * rows * positions,
            bytes_accessed=10 * rows * heads * head_size,
        ),
        compiler_params=pltpu.CompilerParams(vmem_limit_bytes=32 << 20),
        name="prefill",
    )(queries, keys, values, residual)


def split_heads(rows_ref, wide_ref, out_ref, first):
    key_heads = out_ref.shape[0]
    count = rows_ref.shape[0]
    wide_ref[:count] = rows_ref[...].astype(jnp.float32)
    for g in range(key_heads):
        part = wide_ref[pl.ds(g, count // key_heads, stride=key_heads), :]
        out_ref[g, first : first + count // key_heads] = part.astype(out_ref.dtype)


def scores_kernel(
    q_ref, old_ref, new_ref, own_ref, cursor_ref,
    p_old_ref, p_new_ref, p_own_ref, inverse_ref, handed_ref,
    wide_ref, keys_ref, sems,
    *, steps, early, late,
):
    heads, rows, head_size = q_ref.shape
    key_heads, own_count, _ = own_ref.shape
    per = heads // key_heads
    take = 4 if per % 4 == 0 else per
    candidates = rows // steps
    factor = head_size ** (-0.5) * log2_e
    past = old_ref.shape[0]
    copies = [
        pltpu.make_async_copy(old_ref, handed_ref.at[:past], sems.at[0]),
        pltpu.make_async_copy(new_ref, handed_ref.at[past:], sems.at[1]),
    ]
    for copy in copies:
        copy.start()
    split_heads(old_ref, wide_ref, keys_ref, 0)
    split_heads(new_ref, wide_ref, keys_ref, past // key_heads)
    positions = keys_ref.shape[1]
    block = take * rows
    limit = jnp.concatenate([cursor_ref[...]] * take, axis=0)
    within = lax.broadcasted_iota(jnp.int32, (block, positions), 1) < limit
    row = lax.rem(lax.broadcasted_iota(jnp.int32, (block, own_count), 0), rows)
    column = lax.broadcasted_iota(jnp.int32, (block, own_count), 1)
    allowed = (lax.rem(row, candidates) == lax.rem(column, candidates)) & (column <= row)
    for first in range(0, heads, take):
        g = first // per
        here = slice(first * rows, first * rows + block)
        q = q_ref[first : first + take].reshape(block, head_size)
        far = jnp.where(within, contract_last(q, keys_ref[g]), -jnp.inf)
        own = jnp.where(allowed, contract_last(q, own_ref[g]), -jnp.inf)
        top = jnp.maximum(
            jnp.max(far, axis=1, keepdims=True), jnp.max(own, axis=1, keepdims=True)
        )
        far = jnp.exp2((far - top) * factor)
        own = jnp.exp2((own - top) * factor)
        total = jnp.sum(far, axis=1, keepdims=True) + jnp.sum(own, axis=1, keepdims=True)
        far = far.astype(jnp.bfloat16)
        for p_ref, chunks in ((p_old_ref, early), (p_new_ref, late)):
            first_column = 0
            for start, stop in chunks:
                columns = slice(first_column, first_column + stop - start)
                p_ref[here, columns] = far[:, start:stop]
                first_column = columns.stop
        p_own_ref[here] = own.astype(jnp.bfloat16)
        inverse_ref[here] = jnp.broadcast_to(1.0 / total, (block, head_size))
    for copy in copies:
        copy.wait()


HBM = pl.BlockSpec(memory_space=pltpu.HBM)
VMEM = pl.BlockSpec(memory_space=pltpu.VMEM)


def length(chunks):
    return sum(stop - start for start, stop in chunks)


def copies_of(refs, chunks, handed_ref, sems):
    copies = []
    for i, (ref, (start, stop)) in enumerate(zip(refs, chunks)):
        per = ref.shape[0] // (stop - start)
        copies.append(
            pltpu.make_async_copy(ref, handed_ref.at[start * per : stop * per], sems.at[i])
        )
        copies[-1].start()
    return copies


def split_all(refs, chunks, wide_ref, out_ref):
    first = 0
    for ref, (start, stop) in zip(refs, chunks):
        split_heads(ref, wide_ref, out_ref, first)
        first += stop - start


def room(mib):
    return pltpu.CompilerParams(vmem_limit_bytes=mib << 20)


def decode_scores(queries, old_keys, new_keys, own_keys, cursor, steps, early, late):
    heads, rows, head_size = queries.shape
    key_heads, own_count, _ = own_keys.shape
    past = old_keys.shape[0] // key_heads
    span = new_keys.shape[0] // key_heads
    every = heads * rows
    return pl.pallas_call(
        functools.partial(scores_kernel, steps=steps, early=early, late=late),
        in_specs=[VMEM] * 5,
        out_specs=[VMEM] * 4 + [HBM],
        out_shape=[
            jax.ShapeDtypeStruct((every, length(early)), jnp.bfloat16),
            jax.ShapeDtypeStruct((every, length(late)), jnp.bfloat16),
            jax.ShapeDtypeStruct((every, own_count), jnp.bfloat16),
            jax.ShapeDtypeStruct((every, head_size), jnp.float32),
            jax.ShapeDtypeStruct((key_heads * (past + span), head_size), jnp.bfloat16),
        ],
        scratch_shapes=[
            pltpu.VMEM(old_keys.shape, jnp.float32),
            pltpu.VMEM((key_heads, past + span, head_size), jnp.bfloat16),
            pltpu.SemaphoreType.DMA((2,)),
        ],
        compiler_params=room(24),
        cost_estimate=pl.CostEstimate(
            flops=8 * every * (past + span) * head_size,
            transcendentals=every * (past + span),
            bytes_accessed=2 * every * (past + span),
        ),
        name="decode_scores",
    )(queries, old_keys, new_keys, own_keys, cursor)


def mix_kernel(*refs, early):
    p_old_ref, p_own_ref, inverse_ref, own_ref, residual_ref = refs[:5]
    chunk_refs = refs[5 : 5 + len(early)]
    base_ref, handed_ref, wide_ref, values_ref, sems = refs[5 + len(early) :]
    rows = residual_ref.shape[0]
    key_heads, _, head_size = own_ref.shape
    heads = p_old_ref.shape[0] // rows
    per = heads // key_heads
    copies = copies_of(chunk_refs, early, handed_ref, sems)
    split_all(chunk_refs, early, wide_ref, values_ref)
    for g in range(key_heads):
        here = slice(g * per * rows, (g + 1) * per * rows)
        mixed = jnp.dot(p_old_ref[here], values_ref[g], preferred_element_type=jnp.float32)
        mixed += jnp.dot(p_own_ref[here], own_ref[g], preferred_element_type=jnp.float32)
        mixed *= inverse_ref[here]
        for h in range(per):
            lanes = slice((g * per + h) * head_size, (g * per + h + 1) * head_size)
            base_ref[:, lanes] = mixed[h * rows : (h + 1) * rows] + residual_ref[:, lanes].astype(
                jnp.float32
            )
    for copy in copies:
        copy.wait()


def decode_mix(p_old, p_own, inverse, own_values, residual, chunk_values, early, positions):
    key_heads, _, head_size = own_values.shape
    most = max(x.shape[0] for x in chunk_values)
    return pl.pallas_call(
        functools.partial(mix_kernel, early=early),
        in_specs=[VMEM] * (5 + len(early)),
        out_specs=[VMEM, HBM],
        out_shape=[
            jax.ShapeDtypeStruct(residual.shape, jnp.float32),
            jax.ShapeDtypeStruct((key_heads * positions, head_size), jnp.bfloat16),
        ],
        scratch_shapes=[
            pltpu.VMEM((most, head_size), jnp.float32),
            pltpu.VMEM((key_heads, length(early), head_size), jnp.bfloat16),
            pltpu.SemaphoreType.DMA((len(early),)),
        ],
        compiler_params=room(16),
        cost_estimate=pl.CostEstimate(
            flops=4 * p_old.shape[0] * p_old.shape[1] * head_size,
            transcendentals=0,
            bytes_accessed=2 * p_old.shape[0] * p_old.shape[1],
        ),
        name="decode_mix",
    )(p_old, p_own, inverse, own_values, residual, *chunk_values)


def finish_kernel(*refs, late):
    p_new_ref, inverse_ref, base_ref = refs[:3]
    chunk_refs = refs[3 : 3 + len(late)]
    hidden_ref, squares_ref, wide_ref, values_ref = refs[3 + len(late) :]
    rows = base_ref.shape[0]
    key_heads, _, head_size = values_ref.shape
    heads = p_new_ref.shape[0] // rows
    per = heads // key_heads
    split_all(chunk_refs, late, wide_ref, values_ref)
    squares = jnp.zeros((rows, head_size), jnp.float32)
    for g in range(key_heads):
        here = slice(g * per * rows, (g + 1) * per * rows)
        mixed = jnp.dot(p_new_ref[here], values_ref[g], preferred_element_type=jnp.float32)
        mixed *= inverse_ref[here]
        for h in range(per):
            lanes = slice((g * per + h) * head_size, (g * per + h + 1) * head_size)
            hidden = mixed[h * rows : (h + 1) * rows] + base_ref[:, lanes]
            hidden_ref[:, lanes] = hidden
            squares += hidden * hidden
    squares = jnp.broadcast_to(jnp.sum(squares, axis=1, keepdims=True), (rows, 128))
    squares_ref[...] = jnp.transpose(squares)[:8]


def decode_finish(p_new, inverse, base, chunk_values, late):
    rows, features = base.shape
    most, head_size = max(x.shape for x in chunk_values)
    key_heads = sum(x.shape[0] for x in chunk_values) // length(late)
    return pl.pallas_call(
        functools.partial(finish_kernel, late=late),
        in_specs=[VMEM] * (3 + len(late)),
        out_specs=[VMEM] * 2,
        out_shape=[
            jax.ShapeDtypeStruct((rows, features), jnp.float32),
            jax.ShapeDtypeStruct((8, rows), jnp.float32),
        ],
        scratch_shapes=[
            pltpu.VMEM((most, head_size), jnp.float32),
            pltpu.VMEM((key_heads, length(late), head_size), jnp.bfloat16),
        ],
        compiler_params=room(8),
        cost_estimate=pl.CostEstimate(
            flops=2 * p_new.shape[0] * p_new.shape[1] * head_size,
            transcendentals=0,
            bytes_accessed=2 * p_new.shape[0] * p_new.shape[1],
        ),
        name="decode_finish",
    )(p_new, inverse, base, *chunk_values)


def append_kernel(*refs, late):
    *chunk_refs, _, _, handed_ref, sems = refs
    for copy in copies_of(chunk_refs, late, handed_ref, sems):
        copy.wait()


def append(part, chunk_values, late, after):
    return pl.pallas_call(
        functools.partial(append_kernel, late=late),
        in_specs=[VMEM] * len(late) + [HBM, VMEM],
        out_specs=HBM,
        out_shape=jax.ShapeDtypeStruct(part.shape, part.dtype),
        scratch_shapes=[pltpu.SemaphoreType.DMA((len(late),))],
        input_output_aliases={len(late): 0},
        compiler_params=room(2),
        cost_estimate=pl.CostEstimate(
            flops=1000000,
            transcendentals=0,
            bytes_accessed=4 * sum(x.size for x in chunk_values),
        ),
        name="append",
    )(*chunk_values, part, after)


def local(
    prompt_keys,
    prompt_values,
    span_queries,
    span_keys,
    span_values,
    prefill_residual,
    decode_queries,
    decode_keys,
    decode_values,
    decode_residual,
    cursor,
    norm_gain,
):
    halfway = lax.axis_size("pair") // 2
    keys_shape = (prompt_keys.shape[1] + span_keys.shape[1],) + prompt_keys.shape[2:]
    width = norm_gain.shape[0] * lax.axis_size("tp")
    old_keys = from_behind(prompt_keys, "pair", halfway)
    new_keys = from_behind(span_keys, "pair", halfway)
    past, span = prompt_values.shape[1], span_values.shape[1]
    late_past, late_span = min(late_rows, past), min(late_rows, span)
    early = ((0, past - late_past), (past, past + span - late_span))
    late = ((past - late_past, past), (past + span - late_span, past + span))
    early, late = [[(a, b) for a, b in chunks if b > a] for chunks in (early, late)]

    def received(chunk):
        start, stop = chunk
        if start < past:
            rows = prompt_values[:, start:stop]
        else:
            rows = span_values[:, start - past : stop - past]
        rows = from_behind(rows, "pair", halfway)[0]
        return rows.reshape(-1, rows.shape[-1])

    early_values = [received(chunk) for chunk in early]
    late_values = [received(chunk) for chunk in late]
    gain_wide = norm_gain.astype(jnp.float32)

    def normed(hidden, squares):
        scale = lax.rsqrt(squares / width + epsilon)
        return (hidden * scale[..., None] * gain_wide).astype(jnp.bfloat16)

    head_major = lambda x: jnp.transpose(x, (1, 0, 2))
    keys = head_major(jnp.concatenate([prompt_keys[0], span_keys[0]], axis=0))
    values = head_major(jnp.concatenate([prompt_values[0], span_values[0]], axis=0))
    hidden, squares = prefill(head_major(span_queries[0]), keys, values, prefill_residual[0])
    prefill_normed = normed(hidden, lax.psum(jnp.sum(squares, axis=1), "tp"))

    steps, candidates, heads, head_size = decode_queries.shape[1:]
    rows = steps * candidates
    flat = lambda x: x[0].reshape(rows, x.shape[3], head_size)
    prefill_normed, decode_queries = lax.optimization_barrier((prefill_normed, decode_queries))
    mixed_rows = lambda x: x[0].reshape(x.shape[1] * x.shape[2], head_size)
    own_values = head_major(flat(decode_values))
    limits = jnp.concatenate([cursor[0]] * steps)[:, None]
    p_old, p_new, p_own, inverse, handed_keys = decode_scores(
        head_major(flat(decode_queries)),
        mixed_rows(old_keys),
        mixed_rows(new_keys),
        head_major(flat(decode_keys)),
        limits,
        steps,
        early,
        late,
    )
    positions, key_heads, _ = keys_shape
    base, part = decode_mix(
        p_old, p_own, inverse, own_values, decode_residual[0].reshape(rows, -1),
        early_values, early, positions,
    )
    hidden, squares = decode_finish(p_new, inverse, base, late_values, late)
    handed_values = append(part, late_values, late, squares)
    squares = sum_over(squares, "tp")
    decode_normed = normed(hidden, squares[0]).reshape(decode_residual.shape)
    whole = lambda x: x.reshape(1, positions, key_heads, head_size)
    return (prefill_normed[None], whole(handed_keys), whole(handed_values), decode_normed)


def solution(mesh):
    whole = P(("groups", "pair"), None, "tp", None)
    step = P(("groups", "pair"), None, None, "tp", None)
    placed = (
        whole,
        whole,
        whole,
        whole,
        whole,
        P(("groups", "pair"), None, "tp"),
        step,
        step,
        step,
        P(("groups", "pair"), None, None, "tp"),
        P(("groups", "pair"), None),
        P("tp"),
    )
    return jax.shard_map(
        local,
        mesh=mesh,
        in_specs=placed,
        out_specs=(
            P(("groups", "pair"), None, "tp"),
            whole,
            whole,
            P(("groups", "pair"), None, None, "tp"),
        ),
        check_vma=False,
    )
```

```python
import functools

import jax
import jax.numpy as jnp
from jax import lax
from jax.experimental import pallas as pl
from jax.experimental.pallas import tpu as pltpu
from jax.sharding import PartitionSpec as P

epsilon = 1e-05
log2_e = 1.4426950408889634
late_rows = 128


def from_behind(value, axis, steps):
    count = lax.axis_size(axis)
    pairs = [(source, (source + steps) % count) for source in range(count)]
    return lax.ppermute(value, axis, pairs)


def sum_over(value, axis):
    count = lax.axis_size(axis)
    if count & (count - 1):
        return lax.psum(value, axis)
    others = [
        lax.ppermute(value, axis, [(i, i ^ step) for i in range(count)])
        for step in range(count - 1, 0, -1)
    ]
    return functools.reduce(jnp.add, others, value)


def contract_last(a, b):
    return lax.dot_general(a, b, (((1,), (1,)), ((), ())), preferred_element_type=jnp.float32)


def prefill_kernel(q_ref, k_ref, v_ref, residual_ref, hidden_ref, squares_ref, *, block, past):
    rows = q_ref.shape[1]
    head_size = q_ref.shape[2]
    factor = head_size ** (-0.5) * log2_e

    @pl.when(pl.program_id(0) == 0)
    def _():
        squares_ref[...] = jnp.zeros_like(squares_ref)

    visible = lax.broadcasted_iota(jnp.int32, (block, block), 1) <= lax.broadcasted_iota(
        jnp.int32, (block, block), 0
    )
    for start in range(0, rows, block):
        here = slice(start, start + block)
        before = past + start
        q = q_ref[0, here]
        far = contract_last(q, k_ref[0, :before])
        near = contract_last(q, k_ref[0, before : before + block])
        near = jnp.where(visible, near, -jnp.inf)
        top = jnp.maximum(
            jnp.max(far, axis=1, keepdims=True), jnp.max(near, axis=1, keepdims=True)
        )
        far = jnp.exp2((far - top) * factor)
        near = jnp.exp2((near - top) * factor)
        total = jnp.sum(far, axis=1, keepdims=True) + jnp.sum(near, axis=1, keepdims=True)
        mixed = jnp.dot(
            far.astype(jnp.bfloat16), v_ref[0, :before], preferred_element_type=jnp.float32
        ) + jnp.dot(
            near.astype(jnp.bfloat16),
            v_ref[0, before : before + block],
            preferred_element_type=jnp.float32,
        )
        hidden = mixed / total + residual_ref[here].astype(jnp.float32)
        hidden_ref[here] = hidden
        squares_ref[here] = squares_ref[here] + hidden * hidden


def prefill(queries, keys, values, residual):
    heads, rows, head_size = queries.shape
    key_heads, positions, _ = keys.shape
    per = heads // key_heads
    block = 256 if rows % 256 == 0 else rows
    return pl.pallas_call(
        functools.partial(prefill_kernel, block=block, past=positions - rows),
        grid=(heads,),
        in_specs=[
            pl.BlockSpec((1, rows, head_size), lambda h: (h, 0, 0)),
            pl.BlockSpec((1, positions, head_size), lambda h: (h // per, 0, 0)),
            pl.BlockSpec((1, positions, head_size), lambda h: (h // per, 0, 0)),
            pl.BlockSpec((rows, head_size), lambda h: (0, h)),
        ],
        out_specs=[
            pl.BlockSpec((rows, head_size), lambda h: (0, h)),
            pl.BlockSpec((rows, head_size), lambda h: (0, 0)),
        ],
        out_shape=[
            jax.ShapeDtypeStruct((rows, heads * head_size), jnp.float32),
            jax.ShapeDtypeStruct((rows, head_size), jnp.float32),
        ],
        cost_estimate=pl.CostEstimate(
            flops=8 * heads * rows * positions * head_size,
            transcendentals=heads * rows * positions,
            bytes_accessed=10 * rows * heads * head_size,
        ),
        compiler_params=pltpu.CompilerParams(vmem_limit_bytes=32 << 20),
        name="prefill",
    )(queries, keys, values, residual)


def split_heads(rows_ref, wide_ref, out_ref, first):
    key_heads = out_ref.shape[0]
    count = rows_ref.shape[0]
    wide_ref[:count] = rows_ref[...].astype(jnp.float32)
    for g in range(key_heads):
        part = wide_ref[pl.ds(g, count // key_heads, stride=key_heads), :]
        out_ref[g, first : first + count // key_heads] = part.astype(out_ref.dtype)


def scores_kernel(
    q_ref, old_ref, new_ref, own_ref, cursor_ref,
    p_old_ref, p_new_ref, p_own_ref, inverse_ref, handed_ref,
    wide_ref, keys_ref, sems,
    *, steps, early, late,
):
    heads, rows, head_size = q_ref.shape
    key_heads, own_count, _ = own_ref.shape
    per = heads // key_heads
    take = 4 if per % 4 == 0 else per
    candidates = rows // steps
    factor = head_size ** (-0.5) * log2_e
    past = old_ref.shape[0]
    copies = [
        pltpu.make_async_copy(old_ref, handed_ref.at[:past], sems.at[0]),
        pltpu.make_async_copy(new_ref, handed_ref.at[past:], sems.at[1]),
    ]
    for copy in copies:
        copy.start()
    split_heads(old_ref, wide_ref, keys_ref, 0)
    split_heads(new_ref, wide_ref, keys_ref, past // key_heads)
    positions = keys_ref.shape[1]
    block = take * rows
    limit = jnp.concatenate([cursor_ref[...]] * take, axis=0)
    within = lax.broadcasted_iota(jnp.int32, (block, positions), 1) < limit
    row = lax.rem(lax.broadcasted_iota(jnp.int32, (block, own_count), 0), rows)
    column = lax.broadcasted_iota(jnp.int32, (block, own_count), 1)
    allowed = (lax.rem(row, candidates) == lax.rem(column, candidates)) & (column <= row)
    for first in range(0, heads, take):
        g = first // per
        here = slice(first * rows, first * rows + block)
        q = q_ref[first : first + take].reshape(block, head_size)
        far = jnp.where(within, contract_last(q, keys_ref[g]), -jnp.inf)
        own = jnp.where(allowed, contract_last(q, own_ref[g]), -jnp.inf)
        top = jnp.maximum(
            jnp.max(far, axis=1, keepdims=True), jnp.max(own, axis=1, keepdims=True)
        )
        far = jnp.exp2((far - top) * factor)
        own = jnp.exp2((own - top) * factor)
        total = jnp.sum(far, axis=1, keepdims=True) + jnp.sum(own, axis=1, keepdims=True)
        inverse = 1.0 / total
        for p_ref, chunks, factor_of in ((p_old_ref, early, 1.0), (p_new_ref, late, inverse)):
            first_column = 0
            for start, stop in chunks:
                columns = slice(first_column, first_column + stop - start)
                p_ref[here, columns] = (far[:, start:stop] * factor_of).astype(jnp.bfloat16)
                first_column = columns.stop
        p_own_ref[here] = own.astype(jnp.bfloat16)
        inverse_ref[here] = jnp.broadcast_to(inverse, (block, head_size))
    for copy in copies:
        copy.wait()


HBM = pl.BlockSpec(memory_space=pltpu.HBM)
VMEM = pl.BlockSpec(memory_space=pltpu.VMEM)


def length(chunks):
    return sum(stop - start for start, stop in chunks)


def copies_of(refs, chunks, handed_ref, sems):
    copies = []
    for i, (ref, (start, stop)) in enumerate(zip(refs, chunks)):
        per = ref.shape[0] // (stop - start)
        copies.append(
            pltpu.make_async_copy(ref, handed_ref.at[start * per : stop * per], sems.at[i])
        )
        copies[-1].start()
    return copies


def split_all(refs, chunks, wide_ref, out_ref):
    first = 0
    for ref, (start, stop) in zip(refs, chunks):
        split_heads(ref, wide_ref, out_ref, first)
        first += stop - start


def room(mib):
    return pltpu.CompilerParams(vmem_limit_bytes=mib << 20)


def decode_scores(queries, old_keys, new_keys, own_keys, cursor, steps, early, late):
    heads, rows, head_size = queries.shape
    key_heads, own_count, _ = own_keys.shape
    past = old_keys.shape[0] // key_heads
    span = new_keys.shape[0] // key_heads
    every = heads * rows
    return pl.pallas_call(
        functools.partial(scores_kernel, steps=steps, early=early, late=late),
        in_specs=[VMEM] * 5,
        out_specs=[VMEM] * 4 + [HBM],
        out_shape=[
            jax.ShapeDtypeStruct((every, length(early)), jnp.bfloat16),
            jax.ShapeDtypeStruct((every, length(late)), jnp.bfloat16),
            jax.ShapeDtypeStruct((every, own_count), jnp.bfloat16),
            jax.ShapeDtypeStruct((every, head_size), jnp.float32),
            jax.ShapeDtypeStruct((key_heads * (past + span), head_size), jnp.bfloat16),
        ],
        scratch_shapes=[
            pltpu.VMEM(old_keys.shape, jnp.float32),
            pltpu.VMEM((key_heads, past + span, head_size), jnp.bfloat16),
            pltpu.SemaphoreType.DMA((2,)),
        ],
        compiler_params=room(24),
        cost_estimate=pl.CostEstimate(
            flops=8 * every * (past + span) * head_size,
            transcendentals=every * (past + span),
            bytes_accessed=2 * every * (past + span),
        ),
        name="decode_scores",
    )(queries, old_keys, new_keys, own_keys, cursor)


def mix_kernel(*refs, early):
    p_old_ref, p_own_ref, inverse_ref, own_ref, residual_ref = refs[:5]
    chunk_refs = refs[5 : 5 + len(early)]
    base_ref, handed_ref, wide_ref, values_ref, sems = refs[5 + len(early) :]
    rows = residual_ref.shape[0]
    key_heads, _, head_size = own_ref.shape
    heads = p_old_ref.shape[0] // rows
    per = heads // key_heads
    copies = copies_of(chunk_refs, early, handed_ref, sems)
    split_all(chunk_refs, early, wide_ref, values_ref)
    for g in range(key_heads):
        here = slice(g * per * rows, (g + 1) * per * rows)
        mixed = jnp.dot(p_old_ref[here], values_ref[g], preferred_element_type=jnp.float32)
        mixed += jnp.dot(p_own_ref[here], own_ref[g], preferred_element_type=jnp.float32)
        mixed *= inverse_ref[here]
        for h in range(per):
            lanes = slice((g * per + h) * head_size, (g * per + h + 1) * head_size)
            base_ref[:, lanes] = mixed[h * rows : (h + 1) * rows] + residual_ref[:, lanes].astype(
                jnp.float32
            )
    for copy in copies:
        copy.wait()


def decode_mix(p_old, p_own, inverse, own_values, residual, chunk_values, early, positions):
    key_heads, _, head_size = own_values.shape
    most = max(x.shape[0] for x in chunk_values)
    return pl.pallas_call(
        functools.partial(mix_kernel, early=early),
        in_specs=[VMEM] * (5 + len(early)),
        out_specs=[VMEM, HBM],
        out_shape=[
            jax.ShapeDtypeStruct(residual.shape, jnp.float32),
            jax.ShapeDtypeStruct((key_heads * positions, head_size), jnp.bfloat16),
        ],
        scratch_shapes=[
            pltpu.VMEM((most, head_size), jnp.float32),
            pltpu.VMEM((key_heads, length(early), head_size), jnp.bfloat16),
            pltpu.SemaphoreType.DMA((len(early),)),
        ],
        compiler_params=room(16),
        cost_estimate=pl.CostEstimate(
            flops=4 * p_old.shape[0] * p_old.shape[1] * head_size,
            transcendentals=0,
            bytes_accessed=2 * p_old.shape[0] * p_old.shape[1],
        ),
        name="decode_mix",
    )(p_old, p_own, inverse, own_values, residual, *chunk_values)


def finish_kernel(*refs, late):
    p_new_ref, base_ref = refs[:2]
    chunk_refs = refs[2 : 2 + len(late)]
    hidden_ref, squares_ref, wide_ref, values_ref = refs[2 + len(late) :]
    rows = base_ref.shape[0]
    key_heads, _, head_size = values_ref.shape
    heads = p_new_ref.shape[0] // rows
    per = heads // key_heads
    split_all(chunk_refs, late, wide_ref, values_ref)
    squares = jnp.zeros((rows, head_size), jnp.float32)
    for g in range(key_heads):
        here = slice(g * per * rows, (g + 1) * per * rows)
        mixed = jnp.dot(p_new_ref[here], values_ref[g], preferred_element_type=jnp.float32)
        for h in range(per):
            lanes = slice((g * per + h) * head_size, (g * per + h + 1) * head_size)
            hidden = mixed[h * rows : (h + 1) * rows] + base_ref[:, lanes]
            hidden_ref[:, lanes] = hidden
            squares += hidden * hidden
    squares = jnp.broadcast_to(jnp.sum(squares, axis=1, keepdims=True), (rows, 128))
    squares_ref[...] = jnp.transpose(squares)[:8]


def decode_finish(p_new, base, chunk_values, late):
    rows, features = base.shape
    most, head_size = max(x.shape for x in chunk_values)
    key_heads = sum(x.shape[0] for x in chunk_values) // length(late)
    return pl.pallas_call(
        functools.partial(finish_kernel, late=late),
        in_specs=[VMEM] * (2 + len(late)),
        out_specs=[VMEM] * 2,
        out_shape=[
            jax.ShapeDtypeStruct((rows, features), jnp.float32),
            jax.ShapeDtypeStruct((8, rows), jnp.float32),
        ],
        scratch_shapes=[
            pltpu.VMEM((most, head_size), jnp.float32),
            pltpu.VMEM((key_heads, length(late), head_size), jnp.bfloat16),
        ],
        compiler_params=room(8),
        cost_estimate=pl.CostEstimate(
            flops=2 * p_new.shape[0] * p_new.shape[1] * head_size,
            transcendentals=0,
            bytes_accessed=2 * p_new.shape[0] * p_new.shape[1],
        ),
        name="decode_finish",
    )(p_new, base, *chunk_values)


def append_kernel(*refs, late):
    *chunk_refs, _, _, handed_ref, sems = refs
    for copy in copies_of(chunk_refs, late, handed_ref, sems):
        copy.wait()


def append(part, chunk_values, late, after):
    return pl.pallas_call(
        functools.partial(append_kernel, late=late),
        in_specs=[VMEM] * len(late) + [HBM, VMEM],
        out_specs=HBM,
        out_shape=jax.ShapeDtypeStruct(part.shape, part.dtype),
        scratch_shapes=[pltpu.SemaphoreType.DMA((len(late),))],
        input_output_aliases={len(late): 0},
        compiler_params=room(2),
        cost_estimate=pl.CostEstimate(
            flops=1000000,
            transcendentals=0,
            bytes_accessed=4 * sum(x.size for x in chunk_values),
        ),
        name="append",
    )(*chunk_values, part, after)


def local(
    prompt_keys,
    prompt_values,
    span_queries,
    span_keys,
    span_values,
    prefill_residual,
    decode_queries,
    decode_keys,
    decode_values,
    decode_residual,
    cursor,
    norm_gain,
):
    halfway = lax.axis_size("pair") // 2
    keys_shape = (prompt_keys.shape[1] + span_keys.shape[1],) + prompt_keys.shape[2:]
    width = norm_gain.shape[0] * lax.axis_size("tp")
    old_keys = from_behind(prompt_keys, "pair", halfway)
    new_keys = from_behind(span_keys, "pair", halfway)
    past, span = prompt_values.shape[1], span_values.shape[1]
    late_past, late_span = min(late_rows, past), min(late_rows, span)
    early = ((0, past - late_past), (past, past + span - late_span))
    late = ((past - late_past, past), (past + span - late_span, past + span))
    early, late = [[(a, b) for a, b in chunks if b > a] for chunks in (early, late)]

    def received(chunk):
        start, stop = chunk
        if start < past:
            rows = prompt_values[:, start:stop]
        else:
            rows = span_values[:, start - past : stop - past]
        rows = from_behind(rows, "pair", halfway)[0]
        return rows.reshape(-1, rows.shape[-1])

    early_values = [received(chunk) for chunk in early]
    late_values = [received(chunk) for chunk in late]
    gain_wide = norm_gain.astype(jnp.float32)

    def normed(hidden, squares):
        scale = lax.rsqrt(squares / width + epsilon)
        return (hidden * scale[..., None] * gain_wide).astype(jnp.bfloat16)

    head_major = lambda x: jnp.transpose(x, (1, 0, 2))
    keys = head_major(jnp.concatenate([prompt_keys[0], span_keys[0]], axis=0))
    values = head_major(jnp.concatenate([prompt_values[0], span_values[0]], axis=0))
    hidden, squares = prefill(head_major(span_queries[0]), keys, values, prefill_residual[0])
    prefill_normed = normed(hidden, lax.psum(jnp.sum(squares, axis=1), "tp"))

    steps, candidates, heads, head_size = decode_queries.shape[1:]
    rows = steps * candidates
    flat = lambda x: x[0].reshape(rows, x.shape[3], head_size)
    prefill_normed, decode_queries = lax.optimization_barrier((prefill_normed, decode_queries))
    mixed_rows = lambda x: x[0].reshape(x.shape[1] * x.shape[2], head_size)
    own_values = head_major(flat(decode_values))
    limits = jnp.concatenate([cursor[0]] * steps)[:, None]
    p_old, p_new, p_own, inverse, handed_keys = decode_scores(
        head_major(flat(decode_queries)),
        mixed_rows(old_keys),
        mixed_rows(new_keys),
        head_major(flat(decode_keys)),
        limits,
        steps,
        early,
        late,
    )
    positions, key_heads, _ = keys_shape
    base, part = decode_mix(
        p_old, p_own, inverse, own_values, decode_residual[0].reshape(rows, -1),
        early_values, early, positions,
    )
    hidden, squares = decode_finish(p_new, base, late_values, late)
    handed_values = append(part, late_values, late, squares)
    squares = sum_over(squares, "tp")
    decode_normed = normed(hidden, squares[0]).reshape(decode_residual.shape)
    whole = lambda x: x.reshape(1, positions, key_heads, head_size)
    return (prefill_normed[None], whole(handed_keys), whole(handed_values), decode_normed)


def solution(mesh):
    whole = P(("groups", "pair"), None, "tp", None)
    step = P(("groups", "pair"), None, None, "tp", None)
    placed = (
        whole,
        whole,
        whole,
        whole,
        whole,
        P(("groups", "pair"), None, "tp"),
        step,
        step,
        step,
        P(("groups", "pair"), None, None, "tp"),
        P(("groups", "pair"), None),
        P("tp"),
    )
    return jax.shard_map(
        local,
        mesh=mesh,
        in_specs=placed,
        out_specs=(
            P(("groups", "pair"), None, "tp"),
            whole,
            whole,
            P(("groups", "pair"), None, None, "tp"),
        ),
        check_vma=False,
    )
```
